32 devices in a mesh: stage: 4 (over z), tp: 8 (over y, x, core).
Axes of the slice: x: 2, y: 2, z: 4, core: 2. Of those that a mesh axis runs over, the one named last changes fastest.
Arguments:
- x: bfloat16 [8, 2048, 1024], P(None, 'tp')
- g: bfloat16 [4, 2, 1024], P('stage')
- w1: bfloat16 [4, 2, 1024, 4096], P('stage', None, None, 'tp')
- w2: bfloat16 [4, 2, 4096, 1024], P('stage', None, 'tp')
Outputs:
- output: bfloat16 [4, 8, 2048, 1024], P('stage', None, 'tp')
All inputs are finite; a program needn't handle non-finite values.
Results may differ from the reference program's by a relative error of at most 0.02.
Values are sent between devices in bfloat16 or wider.
A program may use at most 1 GiB of HBM per device.

```python
import jax
import jax.numpy as jnp
from jax import lax

STAGES = 4
BLOCKS = 2
M = 8
T = 2048
D = 1024
FF = 4096

EPS = 1e-5


def setup_inputs(seed: int = 0) -> dict:
    k = jax.random.split(jax.random.key(seed), 4)
    x = jax.random.normal(k[0], (M, T, D), jnp.float32)
    g = 1.0 + 0.2 * jax.random.normal(k[1], (STAGES, BLOCKS, D), jnp.float32)
    w1 = jax.random.normal(k[2], (STAGES, BLOCKS, D, FF), jnp.float32) * D ** -0.5
    w2 = jax.random.normal(k[3], (STAGES, BLOCKS, FF, D), jnp.float32) * FF ** -0.5
    return {'x': x.astype(jnp.bfloat16), 'g': g.astype(jnp.bfloat16),
            'w1': w1.astype(jnp.bfloat16), 'w2': w2.astype(jnp.bfloat16)}


def _block(y, g, w1, w2):
    yf = y.astype(jnp.float32)
    mu = jnp.mean(yf, axis=-1, keepdims=True)
    var = jnp.mean(jnp.square(yf - mu), axis=-1, keepdims=True)
    h = ((yf - mu) * lax.rsqrt(var + EPS) * g.astype(jnp.float32)).astype(jnp.bfloat16)
    a = jax.nn.gelu(jnp.dot(h, w1, preferred_element_type=jnp.float32)).astype(jnp.bfloat16)
    return (yf + jnp.dot(a, w2, preferred_element_type=jnp.float32)).astype(jnp.bfloat16)


def reference(x, g, w1, w2):
    def one(xm):
        y = xm
        outs = []
        for s in range(STAGES):
            for b in range(BLOCKS):
                y = _block(y, g[s, b], w1[s, b], w2[s, b])
            outs.append(y)
        return jnp.stack(outs)
    return jnp.transpose(lax.map(one, x), (1, 0, 2, 3))
```

```python
import jax
import jax.numpy as jnp
from jax import lax
from jax.sharding import PartitionSpec as P

EPS = 1e-5


def _ln(y, g):
    yf = y.astype(jnp.float32)
    mu = jnp.mean(yf, axis=-1, keepdims=True)
    var = jnp.mean(jnp.square(yf - mu), axis=-1, keepdims=True)
    return ((yf - mu) * lax.rsqrt(var + EPS) * g.astype(jnp.float32)).astype(jnp.bfloat16)


def _block(y, g, w1, w2):
    h = _ln(y, g)
    a = jax.nn.gelu(jnp.dot(h, w1, preferred_element_type=jnp.float32)).astype(jnp.bfloat16)
    r = jnp.dot(a, w2, preferred_element_type=jnp.float32)
    return (y.astype(jnp.float32) + r).astype(jnp.bfloat16)


def solution(mesh):
    S = mesh.shape['stage']
    fwd = [(i, i + 1) for i in range(S - 1)]
    lag = 2

    def local(x, g, w1, w2):
        s = lax.axis_index('stage')
        M = x.shape[0]
        nb = g.shape[1]
        full1 = [lax.all_gather(w1[0, b], 'tp', axis=1, tiled=True) for b in range(nb)]
        full2 = [lax.all_gather(w2[0, b], 'tp', axis=0, tiled=True) for b in range(nb)]
        steps = M + lag * (S - 1)
        outs, sent = [], []
        for k in range(steps):
            xin = x[min(k, M - 1)]
            y = jnp.where(s == 0, xin, sent[k - lag]) if k >= lag else xin
            for b in range(nb):
                y = _block(y, g[0, b], full1[b], full2[b])
            outs.append(y)
            if k < steps - lag:
                sent.append(lax.ppermute(y, 'stage', fwd))
        out = lax.dynamic_slice_in_dim(jnp.stack(outs), lag * s, M, axis=0)
        return out[None]

    return jax.shard_map(
        local, mesh=mesh,
        in_specs=(P(None, 'tp', None), P('stage', None, None),
                  P('stage', None, None, 'tp'), P('stage', None, 'tp', None)),
        out_specs=P('stage', None, 'tp', None), check_vma=False)
```

```python
import functools

import jax
import jax.numpy as jnp
from jax import lax
from jax.experimental import pallas as pl
from jax.experimental.pallas import tpu as pltpu
from jax.sharding import PartitionSpec as P

EPS = 1e-5
MESH = pl.DeviceIdType.MESH
ROWS = 32


def _kernel(x_hbm, g_ref, w1_hbm, w2_hbm, out_hbm, w1v, w2v, inbuf, hbuf, ybuf, acc, abuf,
            xsem, lsem, rsem, ssem, fsem, zrsem, zssem, osem, *, S):
    s = lax.axis_index('stage')
    tp = lax.axis_index('tp')
    c = tp % 2
    sib = tp + 1 - 2 * c
    nbr = (tp + 2 - 4 * ((tp // 2) % 2), tp + 4 - 8 * (tp // 4))
    NB, _, _, D, U = w1v.shape
    M, T, _ = inbuf.shape

    def slot(b, j, k):
        return w1v.at[b, j, k], w2v.at[b, j, pl.ds(pl.multiple_of(k * U, U), U)]

    def load(b, q):
        d1, d2 = slot(b, 0, 2 * c + q)
        return (pltpu.make_async_copy(w1_hbm.at[0, b, :, pl.ds(q * U, U)], d1, lsem.at[b, q, 0]),
                pltpu.make_async_copy(w2_hbm.at[0, b, pl.ds(q * U, U)], d2, lsem.at[b, q, 1]))

    def copies(src, dst, ssems, rsems, to):
        return tuple(pltpu.make_async_remote_copy(
            src_ref=src[w], dst_ref=dst[w], send_sem=ssems.at[w], recv_sem=rsems.at[w],
            device_id=(s, to), device_id_type=MESH) for w in range(2))

    def send(b, j, l):
        src = slot(b, 0, 2 * c + l) if j == 1 else (
            slot(b, 0, 2 * c + 1 - l) if j == 2 else slot(b, 1, 2 * c + 1 - l))
        return copies(src, slot(b, j, 2 * c + l), ssem.at[b, j - 1, l], rsem.at[b, j, 2 * c + l], nbr[l])

    def share(b, j, l):
        u = slot(b, j, 2 * c + l)
        return copies(u, u, fsem.at[b, j, l], rsem.at[b, j, 2 * c + l], sib)

    def arrived(b, j, k):
        u = slot(b, j, k)
        for cp in copies(u, u, fsem.at[b, j, 0], rsem.at[b, j, k], sib):
            cp.wait_recv()

    def start(cps):
        for cp in cps:
            cp.start()

    def zsend(m):
        return pltpu.make_async_remote_copy(
            src_ref=ybuf.at[m], dst_ref=inbuf.at[m], send_sem=zssem.at[m], recv_sem=zrsem.at[m],
            device_id=(s + 1, tp), device_id_type=MESH)

    def out(m):
        return pltpu.make_async_copy(ybuf.at[m], out_hbm.at[0, m], osem.at[m])

    xin = pltpu.make_async_copy(x_hbm, inbuf, xsem)

    @pl.when(s == 0)
    def _():
        xin.start()
    for b in range(NB):
        for q in range(2):
            start(load(b, q))

    barrier = pltpu.get_barrier_semaphore()
    for to in (sib, *nbr):
        pl.semaphore_signal(barrier, inc=1, device_id=(s, to), device_id_type=MESH)

    @pl.when(s > 0)
    def _():
        pl.semaphore_signal(barrier, inc=1, device_id=(s - 1, tp), device_id_type=MESH)

    @pl.when(s < S - 1)
    def _():
        pl.semaphore_signal(barrier, inc=1, device_id=(s + 1, tp), device_id_type=MESH)
    edge = (s == 0) | (s == S - 1)

    @pl.when(edge)
    def _():
        pl.semaphore_wait(barrier, 4)

    @pl.when(jnp.logical_not(edge))
    def _():
        pl.semaphore_wait(barrier, 5)

    def own(b):
        for q in range(2):
            for cp in load(b, q):
                cp.wait()
        for j in (1, 2):
            for l in range(2):
                start(send(b, j, l))
        for l in range(2):
            start(share(b, 0, l))

    def relay(b, j):
        for l in range(2):
            arrived(b, j, 2 * c + l)
        if j == 1:
            for l in range(2):
                start(send(b, 3, l))
        for l in range(2):
            start(share(b, j, l))
        if j == 1 and b + 1 < NB:
            own(b + 1)

    def others(b, j):
        for l in range(2):
            arrived(b, j, 2 * (1 - c) + l)

    def norm(m, b, y_ref):
        g = g_ref[0, pl.ds(b, 1), :].astype(jnp.float32)
        for r in range(0, T, ROWS):
            rows = pl.ds(r, ROWS)
            yf = y_ref[m, rows, :].astype(jnp.bfloat16).astype(jnp.float32)
            acc[m, rows, :] = yf
            yc = yf - jnp.mean(yf, axis=-1, keepdims=True)
            var = jnp.mean(jnp.square(yc), axis=-1, keepdims=True)
            hbuf[m, rows, :] = (yc * lax.rsqrt(var + EPS) * g).astype(jnp.bfloat16)

    def mlp(m, b, j):
        h = hbuf[m]
        for k in range(4):
            z = jnp.dot(h, w1v[b, j, k], preferred_element_type=jnp.float32)
            abuf[:, k * U:(k + 1) * U] = jax.nn.gelu(z).astype(jnp.bfloat16)
        acc[m] += jnp.dot(abuf[...], w2v[b, j], preferred_element_type=jnp.float32)

    def finish(m):
        ybuf[m] = acc[m].astype(jnp.bfloat16)
        out(m).start()

        @pl.when(s < S - 1)
        def _():
            zsend(m).start()

    def each(body):
        def step(m, carry):
            body(m)
            return carry
        lax.fori_loop(0, M, step, 0)

    own(0)

    @pl.when(s == 0)
    def _():
        xin.wait()
        each(lambda m: norm(m, 0, inbuf))
        for b in range(NB):
            for j in range(4):
                if j:
                    relay(b, j)
                others(b, j)

                def body(m, b=b, j=j):
                    mlp(m, b, j)
                    if j == 3 and b < NB - 1:
                        norm(m, b + 1, acc)
                    if j == 3 and b == NB - 1:
                        finish(m)
                each(body)

    @pl.when(s > 0)
    def _():
        for b in range(NB):
            for j in range(1, 4):
                relay(b, j)
        for b in range(NB):
            for j in range(4):
                others(b, j)

        def body(m):
            pltpu.make_async_remote_copy(
                src_ref=ybuf.at[m], dst_ref=inbuf.at[m], send_sem=zssem.at[m], recv_sem=zrsem.at[m],
                device_id=(s, tp), device_id_type=MESH).wait_recv()
            for b in range(NB):
                norm(m, b, inbuf if b == 0 else acc)

                def step(j, carry, b=b):
                    mlp(m, b, j)
                    return carry
                lax.fori_loop(0, 4, step, 0)
            finish(m)
        each(body)

    for b in range(NB):
        for l in range(2):
            for j in range(4):
                for cp in share(b, j, l):
                    cp.wait_send()
                if j:
                    for cp in send(b, j, l):
                        cp.wait_send()
    for m in range(M):
        out(m).wait()

    @pl.when(s < S - 1)
    def _():
        for m in range(M):
            zsend(m).wait_send()


def solution(mesh):
    S = mesh.shape['stage']

    def local(x, g, w1, w2):
        M, T, D = x.shape
        NB, F = w1.shape[1], w1.shape[3]
        U = F // 2
        bf, f32 = jnp.bfloat16, jnp.float32
        dma = pltpu.SemaphoreType.DMA
        return pl.pallas_call(
            functools.partial(_kernel, S=S),
            out_shape=jax.ShapeDtypeStruct((1, M, T, D), bf),
            in_specs=[pl.BlockSpec(memory_space=pl.ANY), pl.BlockSpec(memory_space=pltpu.VMEM),
                      pl.BlockSpec(memory_space=pl.ANY), pl.BlockSpec(memory_space=pl.ANY)],
            out_specs=pl.BlockSpec(memory_space=pl.ANY),
            scratch_shapes=[
                pltpu.VMEM((NB, 4, 4, D, U), bf), pltpu.VMEM((NB, 4, 4 * U, D), bf),
                pltpu.VMEM((M, T, D), bf), pltpu.VMEM((M, T, D), bf), pltpu.VMEM((M, T, D), bf),
                pltpu.VMEM((M, T, D), f32), pltpu.VMEM((T, 4 * U), bf),
                dma(()), dma((NB, 2, 2)), dma((NB, 4, 4, 2)), dma((NB, 3, 2, 2)), dma((NB, 4, 2, 2)),
                dma((M,)), dma((M,)), dma((M,)),
            ],
            compiler_params=pltpu.CompilerParams(
                collective_id=0, has_side_effects=True, vmem_limit_bytes=67043328),
        )(x, g, w1, w2)

    return jax.shard_map(
        local, mesh=mesh,
        in_specs=(P(None, 'tp', None), P('stage', None, None),
                  P('stage', None, None, 'tp'), P('stage', None, 'tp', None)),
        out_specs=P('stage', None, 'tp', None), check_vma=False)
```

```python
import functools

import jax
import jax.numpy as jnp
from jax import lax
from jax.experimental import pallas as pl
from jax.experimental.pallas import tpu as pltpu
from jax.sharding import PartitionSpec as P

EPS = 1e-5
MESH = pl.DeviceIdType.MESH
ROWS = 32
SPLIT = 2


def _kernel(x_hbm, g_ref, w1_hbm, w2_hbm, out_hbm, w1v, w2v, inbuf, hbuf, ybuf, acc, abuf,
            xsem, lsem, rsem, ssem, fsem, zrsem, zssem, osem, *, S):
    s = lax.axis_index('stage')
    tp = lax.axis_index('tp')
    c = tp % 2
    sib = tp + 1 - 2 * c
    nbr = (tp + 2 - 4 * ((tp // 2) % 2), tp + 4 - 8 * (tp // 4))
    NB, _, _, D, U = w1v.shape
    M, T, _ = inbuf.shape

    def slot(b, j, k):
        return w1v.at[b, j, k], w2v.at[b, j, pl.ds(pl.multiple_of(k * U, U), U)]

    def load(b, q):
        d1, d2 = slot(b, 0, 2 * c + q)
        return (pltpu.make_async_copy(w1_hbm.at[0, b, :, pl.ds(q * U, U)], d1, lsem.at[b, q, 0]),
                pltpu.make_async_copy(w2_hbm.at[0, b, pl.ds(q * U, U)], d2, lsem.at[b, q, 1]))

    def copies(src, dst, ssems, rsems, to):
        return tuple(pltpu.make_async_remote_copy(
            src_ref=src[w], dst_ref=dst[w], send_sem=ssems.at[w], recv_sem=rsems.at[w],
            device_id=(s, to), device_id_type=MESH) for w in range(2))

    def send(b, j, l):
        src = slot(b, 0, 2 * c + l) if j == 1 else (
            slot(b, 0, 2 * c + 1 - l) if j == 2 else slot(b, 1, 2 * c + 1 - l))
        return copies(src, slot(b, j, 2 * c + l), ssem.at[b, j - 1, l], rsem.at[b, j, 2 * c + l], nbr[l])

    def share(b, j, l):
        u = slot(b, j, 2 * c + l)
        return copies(u, u, fsem.at[b, j, l], rsem.at[b, j, 2 * c + l], sib)

    def arrived(b, j, k):
        u = slot(b, j, k)
        for cp in copies(u, u, fsem.at[b, j, 0], rsem.at[b, j, k], sib):
            cp.wait_recv()

    def start(cps):
        for cp in cps:
            cp.start()

    def zsend(m):
        return pltpu.make_async_remote_copy(
            src_ref=ybuf.at[m], dst_ref=inbuf.at[m], send_sem=zssem.at[m], recv_sem=zrsem.at[m],
            device_id=(s + 1, tp), device_id_type=MESH)

    def out(m):
        return pltpu.make_async_copy(ybuf.at[m], out_hbm.at[0, m], osem.at[m])

    xin = pltpu.make_async_copy(x_hbm, inbuf, xsem)

    @pl.when(s == 0)
    def _():
        xin.start()
    for b in range(NB):
        for q in range(2):
            start(load(b, q))

    barrier = pltpu.get_barrier_semaphore()
    for to in (sib, *nbr):
        pl.semaphore_signal(barrier, inc=1, device_id=(s, to), device_id_type=MESH)

    @pl.when(s > 0)
    def _():
        pl.semaphore_signal(barrier, inc=1, device_id=(s - 1, tp), device_id_type=MESH)

    @pl.when(s < S - 1)
    def _():
        pl.semaphore_signal(barrier, inc=1, device_id=(s + 1, tp), device_id_type=MESH)
    edge = (s == 0) | (s == S - 1)

    @pl.when(edge)
    def _():
        pl.semaphore_wait(barrier, 4)

    @pl.when(jnp.logical_not(edge))
    def _():
        pl.semaphore_wait(barrier, 5)

    def own(b):
        for q in range(2):
            for cp in load(b, q):
                cp.wait()
        for j in (1, 2):
            for l in range(2):
                start(send(b, j, l))
        for l in range(2):
            start(share(b, 0, l))

    def relay(b, j):
        for l in range(2):
            arrived(b, j, 2 * c + l)
        if j == 1:
            for l in range(2):
                start(send(b, 3, l))
        for l in range(2):
            start(share(b, j, l))
        if j == 1 and b + 1 < NB:
            own(b + 1)

    def others(b, j):
        for l in range(2):
            arrived(b, j, 2 * (1 - c) + l)

    def norm(m, b, y_ref):
        g = g_ref[0, pl.ds(b, 1), :].astype(jnp.float32)
        for r in range(0, T, ROWS):
            rows = pl.ds(r, ROWS)
            yf = y_ref[m, rows, :].astype(jnp.bfloat16).astype(jnp.float32)
            acc[m, rows, :] = yf
            yc = yf - jnp.mean(yf, axis=-1, keepdims=True)
            var = jnp.mean(jnp.square(yc), axis=-1, keepdims=True)
            hbuf[m, rows, :] = (yc * lax.rsqrt(var + EPS) * g).astype(jnp.bfloat16)

    def mlp(m, b, steps):
        h = hbuf[m]
        n = len(steps) * 4 * U
        for i, j in enumerate(steps):
            for k in range(4):
                z = jnp.dot(h, w1v[b, j, k], preferred_element_type=jnp.float32)
                abuf[:, (4 * i + k) * U:(4 * i + k + 1) * U] = jax.nn.gelu(z).astype(jnp.bfloat16)
        w2 = w2v[b, steps[0]:steps[0] + len(steps)].reshape(n, D)
        acc[m] += jnp.dot(abuf[:, :n], w2, preferred_element_type=jnp.float32)

    def finish(m):
        ybuf[m] = acc[m].astype(jnp.bfloat16)
        out(m).start()

        @pl.when(s < S - 1)
        def _():
            zsend(m).start()

    def each(body):
        def step(m, carry):
            body(m)
            return carry
        lax.fori_loop(0, M, step, 0)

    own(0)

    @pl.when(s == 0)
    def _():
        xin.wait()
        each(lambda m: norm(m, 0, inbuf))
        for b in range(NB):
            for j in range(4):
                if j:
                    relay(b, j)
                others(b, j)

                def body(m, b=b, j=j):
                    mlp(m, b, (j,))
                    if j == 3 and b < NB - 1:
                        norm(m, b + 1, acc)
                    if j == 3 and b == NB - 1:
                        finish(m)
                each(body)

    @pl.when(s > 0)
    def _():
        for b in range(NB):
            for j in range(1, 4):
                relay(b, j)
        for b in range(NB):
            for j in range(4):
                others(b, j)

        def body(m):
            pltpu.make_async_remote_copy(
                src_ref=ybuf.at[m], dst_ref=inbuf.at[m], send_sem=zssem.at[m], recv_sem=zrsem.at[m],
                device_id=(s, tp), device_id_type=MESH).wait_recv()
            for b in range(NB):
                norm(m, b, inbuf if b == 0 else acc)
                mlp(m, b, (0, 1, 2, 3))
            finish(m)
        each(body)

    for b in range(NB):
        for l in range(2):
            for j in range(4):
                for cp in share(b, j, l):
                    cp.wait_send()
                if j:
                    for cp in send(b, j, l):
                        cp.wait_send()
    for m in range(M):
        out(m).wait()

    @pl.when(s < S - 1)
    def _():
        for m in range(M):
            zsend(m).wait_send()


def solution(mesh):
    S = mesh.shape['stage']

    def local(x, g, w1, w2):
        M, T, D = x.shape
        M, T = M * SPLIT, T // SPLIT
        x = x.reshape(M, T, D)
        NB, F = w1.shape[1], w1.shape[3]
        U = F // 2
        bf, f32 = jnp.bfloat16, jnp.float32
        dma = pltpu.SemaphoreType.DMA
        y = pl.pallas_call(
            functools.partial(_kernel, S=S),
            out_shape=jax.ShapeDtypeStruct((1, M, T, D), bf),
            in_specs=[pl.BlockSpec(memory_space=pl.ANY), pl.BlockSpec(memory_space=pltpu.VMEM),
                      pl.BlockSpec(memory_space=pl.ANY), pl.BlockSpec(memory_space=pl.ANY)],
            out_specs=pl.BlockSpec(memory_space=pl.ANY),
            scratch_shapes=[
                pltpu.VMEM((NB, 4, 4, D, U), bf), pltpu.VMEM((NB, 4, 4 * U, D), bf),
                pltpu.VMEM((M, T, D), bf), pltpu.VMEM((M, T, D), bf), pltpu.VMEM((M, T, D), bf),
                pltpu.VMEM((M, T, D), f32), pltpu.VMEM((T, 16 * U), bf),
                dma(()), dma((NB, 2, 2)), dma((NB, 4, 4, 2)), dma((NB, 3, 2, 2)), dma((NB, 4, 2, 2)),
                dma((M,)), dma((M,)), dma((M,)),
            ],
            compiler_params=pltpu.CompilerParams(
                collective_id=0, has_side_effects=True, vmem_limit_bytes=67043328),
        )(x, g, w1, w2)
        return y.reshape(1, M // SPLIT, T * SPLIT, D)

    return jax.shard_map(
        local, mesh=mesh,
        in_specs=(P(None, 'tp', None), P('stage', None, None),
                  P('stage', None, None, 'tp'), P('stage', None, 'tp', None)),
        out_specs=P('stage', None, 'tp', None), check_vma=False)
```

```python
import functools

import jax
import jax.numpy as jnp
from jax import lax
from jax.experimental import pallas as pl
from jax.experimental.pallas import tpu as pltpu
from jax.sharding import PartitionSpec as P

EPS = 1e-5
MESH = pl.DeviceIdType.MESH
ROWS = 32
SPLIT = 2


def _kernel(x_hbm, g_ref, w1_hbm, w2_hbm, out_hbm, w1v, w2v, inbuf, hbuf, ybuf, acc, abuf, up1, up2, over1, over2,
            xsem, lsem, rsem, ssem, fsem, usem, osem2, oss, dss, zrsem, zssem, osem, *, S):
    s = lax.axis_index('stage')
    tp = lax.axis_index('tp')
    c = tp % 2
    sib = tp + 1 - 2 * c
    nbr = (tp + 2 - 4 * ((tp // 2) % 2), tp + 4 - 8 * (tp // 4))
    NB, _, _, D, U = w1v.shape
    M, T, _ = inbuf.shape
    LW = [(l, w) for w in range(2) for l in range(2)]

    def slot(b, j, k, w):
        if w == 0:
            return w1v.at[b, j, k]
        return w2v.at[b, j, pl.ds(pl.multiple_of(k * U, U), U)]

    def load(b, q, w):
        src = w1_hbm.at[0, b, :, pl.ds(q * U, U)] if w == 0 else w2_hbm.at[0, b, pl.ds(q * U, U)]
        return pltpu.make_async_copy(src, slot(b, 0, 2 * c + q, w), lsem.at[b, q, w])

    def remote(src, dst, ssem_, rsem_, stage, to):
        return pltpu.make_async_remote_copy(src_ref=src, dst_ref=dst, send_sem=ssem_, recv_sem=rsem_,
                                            device_id=(stage, to), device_id_type=MESH)

    def send(b, j, l, w):
        src = (slot(b, 0, 2 * c + l, w), slot(b, 0, 2 * c + 1 - l, w), slot(b, 1, 2 * c + 1 - l, w))[j - 1]
        return remote(src, slot(b, j, 2 * c + l, w), ssem.at[b, j - 1, l, w], rsem.at[b, j, 2 * c + l, w], s, nbr[l])

    def share(b, j, l, w):
        u = slot(b, j, 2 * c + l, w)
        return remote(u, u, fsem.at[b, j, l, w], rsem.at[b, j, 2 * c + l, w], s, sib)

    def arrived(b, j, k, w):
        u = slot(b, j, k, w)
        remote(u, u, fsem.at[b, j, 0, w], rsem.at[b, j, k, w], s, sib).wait_recv()

    def helped(w):
        return (s >= w) & (s < S - 1)

    def helper(w):
        return s >= w + 1

    up, over = (up1, up2), (over1, over2)

    def go_up(l, w):
        return remote(slot(1, 0, 2 * c + 1 - l, w), up[w].at[l], ssem.at[1, 1, l, w], usem.at[l, w], s + 1, tp)

    def go_over(l, w):
        return remote(up[w].at[l], over[w].at[l], oss.at[l, w], osem2.at[l, w], s, nbr[l])

    def go_down(l, w):
        return remote(over[w].at[l], slot(1, 2, 2 * c + l, w), dss.at[l, w], rsem.at[1, 2, 2 * c + l, w], s - 1, tp)

    def zsend(m):
        return remote(ybuf.at[m], inbuf.at[m], zssem.at[m], zrsem.at[m], s + 1, tp)

    def out(m):
        return pltpu.make_async_copy(ybuf.at[m], out_hbm.at[0, m], osem.at[m])

    xin = pltpu.make_async_copy(x_hbm, inbuf, xsem)
    for b in range(NB):
        for q in range(2):
            for w in range(2):
                load(b, q, w).start()

    @pl.when(s == 0)
    def _():
        xin.start()

    barrier = pltpu.get_barrier_semaphore()
    for to in (sib, *nbr):
        pl.semaphore_signal(barrier, inc=1, device_id=(s, to), device_id_type=MESH)

    @pl.when(s > 0)
    def _():
        pl.semaphore_signal(barrier, inc=1, device_id=(s - 1, tp), device_id_type=MESH)

    @pl.when(s < S - 1)
    def _():
        pl.semaphore_signal(barrier, inc=1, device_id=(s + 1, tp), device_id_type=MESH)
    edge = (s == 0) | (s == S - 1)

    @pl.when(edge)
    def _():
        pl.semaphore_wait(barrier, 4)

    @pl.when(jnp.logical_not(edge))
    def _():
        pl.semaphore_wait(barrier, 5)

    for l, w in LW:
        load(0, l, w).wait()
    for j in (1, 2):
        for l, w in LW:
            send(0, j, l, w).start()
    for l, w in LW:
        load(1, l, w).wait()
    for w in range(2):
        @pl.when(helped(w))
        def _(w=w):
            for l in range(2):
                go_up(l, w).start()
    for b in range(NB):
        for l, w in LW:
            share(b, 0, l, w).start()

    def own_next():
        for l, w in LW:
            send(1, 1, l, w).start()
        for w in range(2):
            @pl.when(jnp.logical_not(helped(w)))
            def _(w=w):
                for l in range(2):
                    send(1, 2, l, w).start()

    def relay(b, j, on):
        for l, w in LW:
            arrived(b, j, 2 * c + l, w)
            if on:
                send(b, 3, 1 - l, w).start()
            share(b, j, l, w).start()

    def others(b, j):
        for l, w in LW:
            arrived(b, j, 2 * (1 - c) + l, w)

    def norm(m, b, y_ref):
        g = g_ref[0, pl.ds(b, 1), :].astype(jnp.float32)
        for r in range(0, T, ROWS):
            rows = pl.ds(r, ROWS)
            yf = y_ref[m, rows, :].astype(jnp.bfloat16).astype(jnp.float32)
            acc[m, rows, :] = yf
            yc = yf - jnp.mean(yf, axis=-1, keepdims=True)
            var = jnp.mean(jnp.square(yc), axis=-1, keepdims=True)
            hbuf[m, rows, :] = (yc * lax.rsqrt(var + EPS) * g).astype(jnp.bfloat16)

    def mlp(m, b, steps):
        h = hbuf[m]
        n = len(steps) * 4 * U
        for i, j in enumerate(steps):
            for k in range(4):
                z = jnp.dot(h, w1v[b, j, k], preferred_element_type=jnp.float32)
                abuf[:, (4 * i + k) * U:(4 * i + k + 1) * U] = jax.nn.gelu(z).astype(jnp.bfloat16)
        w2 = w2v[b, steps[0]:steps[0] + len(steps)].reshape(n, D)
        acc[m] += jnp.dot(abuf[:, :n], w2, preferred_element_type=jnp.float32)

    def finish(m):
        ybuf[m] = acc[m].astype(jnp.bfloat16)
        out(m).start()

        @pl.when(s < S - 1)
        def _():
            zsend(m).start()

    def each(body):
        def step(m, carry):
            body(m)
            return carry
        lax.fori_loop(0, M, step, 0)

    @pl.when(s == 0)
    def _():
        xin.wait()
        each(lambda m: norm(m, 0, inbuf))
        for b in range(NB):
            for j in range(4):
                if j:
                    relay(b, j, j == 1)
                if (b, j) == (0, 1):
                    own_next()
                others(b, j)

                def body(m, b=b, j=j):
                    mlp(m, b, (j,))
                    if j == 3 and b < NB - 1:
                        norm(m, b + 1, acc)
                    if j == 3 and b == NB - 1:
                        finish(m)
                each(body)

    @pl.when(s > 0)
    def _():
        relay(0, 1, False)
        for w in range(2):
            @pl.when(helper(w))
            def _(w=w):
                for l in range(2):
                    go_up(l, w).wait_recv()
                    go_over(l, w).start()
        for l, w in LW:
            send(0, 3, l, w).start()
        own_next()
        relay(0, 2, False)
        for w in range(2):
            @pl.when(helper(w))
            def _(w=w):
                for l in range(2):
                    go_over(l, w).wait_recv()
                    go_down(l, w).start()
        relay(0, 3, False)
        relay(1, 1, True)
        relay(1, 2, False)
        relay(1, 3, False)
        for b in range(NB):
            for j in range(4):
                others(b, j)

        def body(m):
            zsend(m).wait_recv()
            for b in range(NB):
                norm(m, b, inbuf if b == 0 else acc)
                mlp(m, b, (0, 1, 2, 3))
            finish(m)
        each(body)

    for b in range(NB):
        for j in range(4):
            for l, w in LW:
                share(b, j, l, w).wait_send()
                if j:
                    send(b, j, l, w).wait_send()
    for w in range(2):
        @pl.when(helper(w))
        def _(w=w):
            for l in range(2):
                go_over(l, w).wait_send()
                go_down(l, w).wait_send()
    for m in range(M):
        out(m).wait()

    @pl.when(s < S - 1)
    def _():
        for m in range(M):
            zsend(m).wait_send()


def solution(mesh):
    S = mesh.shape['stage']

    def local(x, g, w1, w2):
        M, T, D = x.shape
        M, T = M * SPLIT, T // SPLIT
        x = x.reshape(M, T, D)
        NB, F = w1.shape[1], w1.shape[3]
        U = F // 2
        bf, f32 = jnp.bfloat16, jnp.float32
        dma = pltpu.SemaphoreType.DMA
        y = pl.pallas_call(
            functools.partial(_kernel, S=S),
            out_shape=jax.ShapeDtypeStruct((1, M, T, D), bf),
            in_specs=[pl.BlockSpec(memory_space=pl.ANY), pl.BlockSpec(memory_space=pltpu.VMEM),
                      pl.BlockSpec(memory_space=pl.ANY), pl.BlockSpec(memory_space=pl.ANY)],
            out_specs=pl.BlockSpec(memory_space=pl.ANY),
            scratch_shapes=[
                pltpu.VMEM((NB, 4, 4, D, U), bf), pltpu.VMEM((NB, 4, 4 * U, D), bf),
                pltpu.VMEM((M, T, D), bf), pltpu.VMEM((M, T, D), bf), pltpu.VMEM((M, T, D), bf),
                pltpu.VMEM((M, T, D), f32), pltpu.VMEM((T, 16 * U), bf),
                pltpu.VMEM((2, D, U), bf), pltpu.VMEM((2, U, D), bf), pltpu.VMEM((2, D, U), bf), pltpu.VMEM((2, U, D), bf),
                dma(()), dma((NB, 2, 2)), dma((NB, 4, 4, 2)), dma((NB, 3, 2, 2)), dma((NB, 4, 2, 2)),
                dma((2, 2)), dma((2, 2)), dma((2, 2)), dma((2, 2)),
                dma((M,)), dma((M,)), dma((M,)),
            ],
            compiler_params=pltpu.CompilerParams(
                collective_id=0, has_side_effects=True, vmem_limit_bytes=67043328),
        )(x, g, w1, w2)
        return y.reshape(1, M // SPLIT, T * SPLIT, D)

    return jax.shard_map(
        local, mesh=mesh,
        in_specs=(P(None, 'tp', None), P('stage', None, None),
                  P('stage', None, None, 'tp'), P('stage', None, 'tp', None)),
        out_specs=P('stage', None, 'tp', None), check_vma=False)
```

```python
import functools

import jax
import jax.numpy as jnp
from jax import lax
from jax.experimental import pallas as pl
from jax.experimental.pallas import tpu as pltpu
from jax.sharding import PartitionSpec as P

EPS = 1e-5
MESH = pl.DeviceIdType.MESH
ROWS = 32
WIDE = 256
CHUNK, EDGE = 128, 64


def _kernel(x_hbm, g_ref, w1_hbm, w2_hbm, out_hbm, w1v, w2v, inbuf, hbuf, ybuf, acc, abuf, up1, up2, over1, over2,
            xsem, lsem, rsem, ssem, fsem, usem, osem2, oss, dss, zrsem, zssem, osem, *, S):
    s = lax.axis_index('stage')
    tp = lax.axis_index('tp')
    c = tp % 2
    sib = tp + 1 - 2 * c
    nbr = (tp + 2 - 4 * ((tp // 2) % 2), tp + 4 - 8 * (tp // 4))
    NB, _, _, D, U = w1v.shape
    R = inbuf.shape[0]
    LW = [(l, w) for w in range(2) for l in range(2)]

    def slot(b, j, k, w):
        if w == 0:
            return w1v.at[b, j, k]
        return w2v.at[b, j, pl.ds(pl.multiple_of(k * U, U), U)]

    def load(b, q, w):
        src = w1_hbm.at[0, b, :, pl.ds(q * U, U)] if w == 0 else w2_hbm.at[0, b, pl.ds(q * U, U)]
        return pltpu.make_async_copy(src, slot(b, 0, 2 * c + q, w), lsem.at[b, q, w])

    def remote(src, dst, ssem_, rsem_, stage, to):
        return pltpu.make_async_remote_copy(src_ref=src, dst_ref=dst, send_sem=ssem_, recv_sem=rsem_,
                                            device_id=(stage, to), device_id_type=MESH)

    def send(b, j, l, w):
        src = (slot(b, 0, 2 * c + l, w), slot(b, 0, 2 * c + 1 - l, w), slot(b, 1, 2 * c + 1 - l, w))[j - 1]
        return remote(src, slot(b, j, 2 * c + l, w), ssem.at[b, j - 1, l, w], rsem.at[b, j, 2 * c + l, w], s, nbr[l])

    def share(b, j, l, w):
        u = slot(b, j, 2 * c + l, w)
        return remote(u, u, fsem.at[b, j, l, w], rsem.at[b, j, 2 * c + l, w], s, sib)

    def arrived(b, j, k, w):
        u = slot(b, j, k, w)
        remote(u, u, fsem.at[b, j, 0, w], rsem.at[b, j, k, w], s, sib).wait_recv()

    def helped(w):
        return (s >= w) & (s < S - 1)

    def helper(w):
        return s >= w + 1

    up, over = (up1, up2), (over1, over2)

    def go_up(l, w):
        return remote(slot(1, 0, 2 * c + 1 - l, w), up[w].at[l], ssem.at[1, 1, l, w], usem.at[l, w], s + 1, tp)

    def go_over(l, w):
        return remote(up[w].at[l], over[w].at[l], oss.at[l, w], osem2.at[l, w], s, nbr[l])

    def go_down(l, w):
        return remote(over[w].at[l], slot(1, 2, 2 * c + l, w), dss.at[l, w], rsem.at[1, 2, 2 * c + l, w], s - 1, tp)

    mid = (R - 2 * EDGE) // CHUNK

    def rows_of(i, n):
        start = (0 if i == 0 else R - EDGE) if n == EDGE else EDGE + CHUNK * (i - 1)
        return pl.ds(start if isinstance(start, int) else pl.multiple_of(start, EDGE), n)

    def zsend(i, n):
        r = rows_of(i, n)
        return remote(ybuf.at[r], inbuf.at[r], zssem.at[i], zrsem.at[i], s + 1, tp)

    def out(i, n):
        r = rows_of(i, n)
        return pltpu.make_async_copy(ybuf.at[r], out_hbm.at[r], osem.at[i])

    def each(body):
        body(0, EDGE)

        def step(i, carry):
            body(i, CHUNK)
            return carry
        lax.fori_loop(1, mid + 1, step, 0)
        body(mid + 1, EDGE)

    xin = pltpu.make_async_copy(x_hbm, inbuf, xsem)
    for b in range(NB):
        for q in range(2):
            for w in range(2):
                load(b, q, w).start()

    @pl.when(s == 0)
    def _():
        xin.start()

    barrier = pltpu.get_barrier_semaphore()
    for to in (sib, *nbr):
        pl.semaphore_signal(barrier, inc=1, device_id=(s, to), device_id_type=MESH)

    @pl.when(s > 0)
    def _():
        pl.semaphore_signal(barrier, inc=1, device_id=(s - 1, tp), device_id_type=MESH)

    @pl.when(s < S - 1)
    def _():
        pl.semaphore_signal(barrier, inc=1, device_id=(s + 1, tp), device_id_type=MESH)
    edge = (s == 0) | (s == S - 1)

    @pl.when(edge)
    def _():
        pl.semaphore_wait(barrier, 4)

    @pl.when(jnp.logical_not(edge))
    def _():
        pl.semaphore_wait(barrier, 5)

    for l, w in LW:
        load(0, l, w).wait()
    for j in (1, 2):
        for l, w in LW:
            send(0, j, l, w).start()
    for l, w in LW:
        load(1, l, w).wait()
    for w in range(2):
        @pl.when(helped(w))
        def _(w=w):
            for l in range(2):
                go_up(l, w).start()
    for b in range(NB):
        for l, w in LW:
            share(b, 0, l, w).start()

    def own_next():
        for l, w in LW:
            send(1, 1, l, w).start()
        for w in range(2):
            @pl.when(jnp.logical_not(helped(w)))
            def _(w=w):
                for l in range(2):
                    send(1, 2, l, w).start()

    def relay(b, j, on):
        for l, w in LW:
            arrived(b, j, 2 * c + l, w)
            if on:
                send(b, 3, 1 - l, w).start()
            share(b, j, l, w).start()

    def others(b, j):
        for l, w in LW:
            arrived(b, j, 2 * (1 - c) + l, w)

    def norm(r0, n, b, y_ref):
        g = g_ref[0, pl.ds(b, 1), :].astype(jnp.float32)
        for r in range(0, n, ROWS):
            rows = pl.ds(r0 + r, ROWS)
            yf = y_ref[rows, :].astype(jnp.bfloat16).astype(jnp.float32)
            acc[rows, :] = yf
            yc = yf - jnp.mean(yf, axis=-1, keepdims=True)
            var = jnp.mean(jnp.square(yc), axis=-1, keepdims=True)
            hbuf[rows, :] = (yc * lax.rsqrt(var + EPS) * g).astype(jnp.bfloat16)

    def mlp(rows, b, steps):
        h = hbuf[rows, :]
        n = len(steps) * 4 * U
        for i, j in enumerate(steps):
            for k in range(4):
                z = jnp.dot(h, w1v[b, j, k], preferred_element_type=jnp.float32)
                abuf[:rows.size, (4 * i + k) * U:(4 * i + k + 1) * U] = jax.nn.gelu(z).astype(jnp.bfloat16)
        w2 = w2v[b, steps[0]:steps[0] + len(steps)].reshape(n, D)
        acc[rows, :] += jnp.dot(abuf[:rows.size, :n], w2, preferred_element_type=jnp.float32)

    def finish(i, n):
        rows = rows_of(i, n)
        ybuf[rows, :] = acc[rows, :].astype(jnp.bfloat16)

        @pl.when(s < S - 1)
        def _():
            zsend(i, n).start()
        out(i, n).start()

    @pl.when(s == 0)
    def _():
        def wide(body):
            def step(i, carry):
                body(pl.multiple_of(i * WIDE, WIDE))
                return carry
            lax.fori_loop(0, R // WIDE, step, 0)

        xin.wait()
        wide(lambda r0: norm(r0, WIDE, 0, inbuf))
        for b in range(NB):
            for j in range(4):
                if j:
                    relay(b, j, j == 1)
                if (b, j) == (0, 2):
                    own_next()
                others(b, j)
                if (b, j) == (NB - 1, 3):
                    def last(i, n):
                        mlp(rows_of(i, n), NB - 1, (3,))
                        finish(i, n)
                    each(last)
                else:
                    def body(r0, b=b, j=j):
                        mlp(pl.ds(r0, WIDE), b, (j,))
                        if j == 3:
                            norm(r0, WIDE, b + 1, acc)
                    wide(body)

    @pl.when(s > 0)
    def _():
        relay(0, 1, False)
        for w in range(2):
            @pl.when(helper(w))
            def _(w=w):
                for l in range(2):
                    go_up(l, w).wait_recv()
                    go_over(l, w).start()
        for l, w in LW:
            send(0, 3, l, w).start()
        relay(0, 2, False)
        for w in range(2):
            @pl.when(helper(w))
            def _(w=w):
                for l in range(2):
                    go_over(l, w).wait_recv()
                    go_down(l, w).start()
            if w == 0:
                own_next()
        relay(0, 3, False)
        relay(1, 1, True)
        relay(1, 2, False)
        relay(1, 3, False)
        for b in range(NB):
            for j in range(4):
                others(b, j)

        def body(i, n):
            zsend(i, n).wait_recv()
            rows = rows_of(i, n)
            for b in range(NB):
                norm(rows.start, n, b, inbuf if b == 0 else acc)
                mlp(rows, b, (0, 1, 2, 3))
            finish(i, n)
        each(body)

    for b in range(NB):
        for j in range(4):
            for l, w in LW:
                share(b, j, l, w).wait_send()
                if j:
                    send(b, j, l, w).wait_send()
    for w in range(2):
        @pl.when(helper(w))
        def _(w=w):
            for l in range(2):
                go_over(l, w).wait_send()
                go_down(l, w).wait_send()

    def ended(i, n):
        out(i, n).wait()

        @pl.when(s < S - 1)
        def _():
            zsend(i, n).wait_send()
    each(ended)


def solution(mesh):
    S = mesh.shape['stage']

    def local(x, g, w1, w2):
        M, T, D = x.shape
        R = M * T
        n = (R - 2 * EDGE) // CHUNK + 2
        NB, F = w1.shape[1], w1.shape[3]
        U = F // 2
        bf, f32 = jnp.bfloat16, jnp.float32
        dma = pltpu.SemaphoreType.DMA
        y = pl.pallas_call(
            functools.partial(_kernel, S=S),
            out_shape=jax.ShapeDtypeStruct((R, D), bf),
            in_specs=[pl.BlockSpec(memory_space=pl.ANY), pl.BlockSpec(memory_space=pltpu.VMEM),
                      pl.BlockSpec(memory_space=pl.ANY), pl.BlockSpec(memory_space=pl.ANY)],
            out_specs=pl.BlockSpec(memory_space=pl.ANY),
            scratch_shapes=[
                pltpu.VMEM((NB, 4, 4, D, U), bf), pltpu.VMEM((NB, 4, 4 * U, D), bf),
                pltpu.VMEM((R, D), bf), pltpu.VMEM((R, D), bf), pltpu.VMEM((R, D), bf),
                pltpu.VMEM((R, D), f32), pltpu.VMEM((WIDE, 16 * U), bf),
                pltpu.VMEM((2, D, U), bf), pltpu.VMEM((2, U, D), bf), pltpu.VMEM((2, D, U), bf), pltpu.VMEM((2, U, D), bf),
                dma(()), dma((NB, 2, 2)), dma((NB, 4, 4, 2)), dma((NB, 3, 2, 2)), dma((NB, 4, 2, 2)),
                dma((2, 2)), dma((2, 2)), dma((2, 2)), dma((2, 2)),
                dma((n,)), dma((n,)), dma((n,)),
            ],
            compiler_params=pltpu.CompilerParams(
                collective_id=0, has_side_effects=True, vmem_limit_bytes=67043328),
        )(x.reshape(R, D), g, w1, w2)
        return y.reshape(1, M, T, D)

    return jax.shard_map(
        local, mesh=mesh,
        in_specs=(P(None, 'tp', None), P('stage', None, None),
                  P('stage', None, None, 'tp'), P('stage', None, 'tp', None)),
        out_specs=P('stage', None, 'tp', None), check_vma=False)
```

```python
import functools

import jax
import jax.numpy as jnp
from jax import lax
from jax.experimental import pallas as pl
from jax.experimental.pallas import tpu as pltpu
from jax.sharding import PartitionSpec as P

EPS = 1e-5
MESH = pl.DeviceIdType.MESH
ROWS = 32
WIDE = 256
CHUNK = 128


def _kernel(x_hbm, g_ref, w1_hbm, w2_hbm, y_ref, w1v, w2v, inbuf, hbuf, acc, abuf, up, over,
            xsem, lsem, rsem, ssem, fsem, usem, ovsem, oss, dss, zrsem, zssem, *, S):
    s = lax.axis_index('stage')
    tp = lax.axis_index('tp')
    c = tp % 2
    sib = tp + 1 - 2 * c
    nbr = (tp + 2 - 4 * ((tp // 2) % 2), tp + 4 - 8 * (tp // 4))
    NB, _, _, D, U = w1v.shape
    R = inbuf.shape[0]
    LW = [(l, w) for w in range(2) for l in range(2)]

    def slot(b, j, k, w):
        if w == 0:
            return w1v.at[b, j, k]
        return w2v.at[b, j, pl.ds(pl.multiple_of(k * U, U), U)]

    def load(b, q, w):
        src = w1_hbm.at[0, b, :, pl.ds(q * U, U)] if w == 0 else w2_hbm.at[0, b, pl.ds(q * U, U)]
        return pltpu.make_async_copy(src, slot(b, 0, 2 * c + q, w), lsem.at[b, q, w])

    def remote(src, dst, ssem_, rsem_, stage, to):
        return pltpu.make_async_remote_copy(src_ref=src, dst_ref=dst, send_sem=ssem_, recv_sem=rsem_,
                                            device_id=(stage, to), device_id_type=MESH)

    def send(b, j, l, w):
        src = (slot(b, 0, 2 * c + l, w), slot(b, 0, 2 * c + 1 - l, w), slot(b, 1, 2 * c + 1 - l, w))[j - 1]
        return remote(src, slot(b, j, 2 * c + l, w), ssem.at[b, j - 1, l, w], rsem.at[b, j, 2 * c + l, w], s, nbr[l])

    def share(b, j, l, w):
        u = slot(b, j, 2 * c + l, w)
        return remote(u, u, fsem.at[b, j, l, w], rsem.at[b, j, 2 * c + l, w], s, sib)

    def arrived(b, j, k, w):
        u = slot(b, j, k, w)
        remote(u, u, fsem.at[b, j, 0, w], rsem.at[b, j, k, w], s, sib).wait_recv()

    helped, helper = s < S - 1, s > 0

    def go_up(l):
        return remote(slot(1, 0, 2 * c + 1 - l, 0), up.at[l], ssem.at[1, 1, l, 0], usem.at[l], s + 1, tp)

    def go_over(l):
        return remote(up.at[l], over.at[l], oss.at[l], ovsem.at[l], s, nbr[l])

    def go_down(l):
        return remote(over.at[l], slot(1, 2, 2 * c + l, 0), dss.at[l], rsem.at[1, 2, 2 * c + l, 0], s - 1, tp)

    def rows_of(i):
        return pl.ds(pl.multiple_of(i * CHUNK, CHUNK), CHUNK)

    def zsend(i):
        r = rows_of(i)
        return remote(y_ref.at[r], inbuf.at[r], zssem.at[i], zrsem.at[i], s + 1, tp)

    def each(n, body):
        def step(i, carry):
            body(i)
            return carry
        lax.fori_loop(0, n, step, 0)

    xin = pltpu.make_async_copy(x_hbm, inbuf, xsem)
    for b in range(NB):
        for q in range(2):
            for w in range(2):
                load(b, q, w).start()

    @pl.when(s == 0)
    def _():
        xin.start()

    barrier = pltpu.get_barrier_semaphore()
    for to in (sib, *nbr):
        pl.semaphore_signal(barrier, inc=1, device_id=(s, to), device_id_type=MESH)

    @pl.when(s > 0)
    def _():
        pl.semaphore_signal(barrier, inc=1, device_id=(s - 1, tp), device_id_type=MESH)

    @pl.when(s < S - 1)
    def _():
        pl.semaphore_signal(barrier, inc=1, device_id=(s + 1, tp), device_id_type=MESH)
    edge = (s == 0) | (s == S - 1)

    @pl.when(edge)
    def _():
        pl.semaphore_wait(barrier, 4)

    @pl.when(jnp.logical_not(edge))
    def _():
        pl.semaphore_wait(barrier, 5)

    for l, w in LW:
        load(0, l, w).wait()
    for j in (1, 2):
        for l, w in LW:
            send(0, j, l, w).start()
    for l, w in LW:
        load(1, l, w).wait()

    @pl.when(helped)
    def _():
        for l in range(2):
            go_up(l).start()
    for b in range(NB):
        for l, w in LW:
            share(b, 0, l, w).start()

    def own_next():
        for l, w in LW:
            send(1, 1, l, w).start()

        @pl.when(jnp.logical_not(helped))
        def _():
            for l in range(2):
                send(1, 2, l, 0).start()
        for l in range(2):
            send(1, 2, l, 1).start()

    def relay(b, j, on):
        for l, w in LW:
            arrived(b, j, 2 * c + l, w)
            if on:
                send(b, 3, 1 - l, w).start()
            share(b, j, l, w).start()

    def others(b, j):
        for l, w in LW:
            arrived(b, j, 2 * (1 - c) + l, w)

    def norm(r0, n, b, src):
        g = g_ref[0, pl.ds(b, 1), :].astype(jnp.float32)
        for r in range(0, n, ROWS):
            rows = pl.ds(r0 + r, ROWS)
            yf = src[rows, :].astype(jnp.bfloat16).astype(jnp.float32)
            acc[rows, :] = yf
            yc = yf - jnp.mean(yf, axis=-1, keepdims=True)
            var = jnp.mean(jnp.square(yc), axis=-1, keepdims=True)
            hbuf[rows, :] = (yc * lax.rsqrt(var + EPS) * g).astype(jnp.bfloat16)

    def mlp(rows, b, j0, steps):
        h = hbuf[rows, :]
        n = steps * 4 * U
        for i in range(steps):
            for k in range(4):
                z = jnp.dot(h, w1v[b, j0 + i, k], preferred_element_type=jnp.float32)
                abuf[:rows.size, (4 * i + k) * U:(4 * i + k + 1) * U] = jax.nn.gelu(z).astype(jnp.bfloat16)
        w2 = w2v[b, j0] if steps == 1 else w2v[b, j0:j0 + steps].reshape(n, D)
        acc[rows, :] += jnp.dot(abuf[:rows.size, :n], w2, preferred_element_type=jnp.float32)

    def finish(i):
        rows = rows_of(i)
        y_ref[rows, :] = acc[rows, :].astype(jnp.bfloat16)

        @pl.when(s < S - 1)
        def _():
            zsend(i).start()

    @pl.when(s == 0)
    def _():
        xin.wait()
        each(R // WIDE, lambda i: norm(pl.multiple_of(i * WIDE, WIDE), WIDE, 0, inbuf))

        def events(b, j):
            if j:
                relay(b, j, j == 1)
            if (b, j) == (0, 2):
                own_next()
            others(b, j)

        def step(t):
            b, j = t // 4, t % 4
            for e in range(4 * NB - 1):
                @pl.when(t == e)
                def _(e=e):
                    events(e // 4, e % 4)

            each(R // WIDE, lambda i: mlp(pl.ds(pl.multiple_of(i * WIDE, WIDE), WIDE), b, j, 1))

            @pl.when(t == 3)
            def _():
                each(R // WIDE, lambda i: norm(pl.multiple_of(i * WIDE, WIDE), WIDE, 1, acc))
        each(4 * NB - 1, step)
        events(NB - 1, 3)

        def last(i):
            mlp(rows_of(i), NB - 1, 3, 1)
            finish(i)
        each(R // CHUNK, last)

    @pl.when(s > 0)
    def _():
        relay(0, 1, False)
        for l in range(2):
            go_up(l).wait_recv()
            go_over(l).start()
        for l, w in LW:
            send(0, 3, l, w).start()
        relay(0, 2, False)
        own_next()
        for l in range(2):
            go_over(l).wait_recv()
            go_down(l).start()
        relay(0, 3, False)
        relay(1, 1, True)
        relay(1, 2, False)
        relay(1, 3, False)
        for b in range(NB):
            for j in range(4):
                others(b, j)

        def body(i):
            zsend(i).wait_recv()
            rows = rows_of(i)
            for b in range(NB):
                norm(rows.start, CHUNK, b, inbuf if b == 0 else acc)
                mlp(rows, b, 0, 4)
            finish(i)
        each(R // CHUNK, body)

    for b in range(NB):
        for j in range(4):
            for l, w in LW:
                share(b, j, l, w).wait_send()
                if j:
                    send(b, j, l, w).wait_send()

    @pl.when(helper)
    def _():
        for l in range(2):
            go_over(l).wait_send()
            go_down(l).wait_send()

    @pl.when(s < S - 1)
    def _():
        each(R // CHUNK, lambda i: zsend(i).wait_send())


def solution(mesh):
    S = mesh.shape['stage']

    def local(x, g, w1, w2):
        M, T, D = x.shape
        R = M * T
        n = R // CHUNK
        NB, F = w1.shape[1], w1.shape[3]
        U = F // 2
        bf, f32 = jnp.bfloat16, jnp.float32
        dma = pltpu.SemaphoreType.DMA
        y = pl.pallas_call(
            functools.partial(_kernel, S=S),
            out_shape=pltpu.VMEM((R, D), bf),
            in_specs=[pl.BlockSpec(memory_space=pl.ANY), pl.BlockSpec(memory_space=pltpu.VMEM),
                      pl.BlockSpec(memory_space=pl.ANY), pl.BlockSpec(memory_space=pl.ANY)],
            out_specs=pl.BlockSpec(memory_space=pltpu.VMEM),
            scratch_shapes=[
                pltpu.VMEM((NB, 4, 4, D, U), bf), pltpu.VMEM((NB, 4, 4 * U, D), bf),
                pltpu.VMEM((R, D), bf), pltpu.VMEM((R, D), bf),
                pltpu.VMEM((R, D), f32), pltpu.VMEM((WIDE, 16 * U), bf),
                pltpu.VMEM((2, D, U), bf), pltpu.VMEM((2, D, U), bf),
                dma(()), dma((NB, 2, 2)), dma((NB, 4, 4, 2)), dma((NB, 3, 2, 2)), dma((NB, 4, 2, 2)),
                dma((2,)), dma((2,)), dma((2,)), dma((2,)),
                dma((n,)), dma((n,)),
            ],
            compiler_params=pltpu.CompilerParams(
                collective_id=0, has_side_effects=True, vmem_limit_bytes=62 * 1000 * 1000),
        )(x.reshape(R, D), g, w1, w2)
        return y.reshape(1, M, T, D)

    return jax.shard_map(
        local, mesh=mesh,
        in_specs=(P(None, 'tp', None), P('stage', None, None),
                  P('stage', None, None, 'tp'), P('stage', None, 'tp', None)),
        out_specs=P('stage', None, 'tp', None), check_vma=False)
```

```python
import functools

import jax
import jax.numpy as jnp
from jax import lax
from jax.experimental import pallas as pl
from jax.experimental.pallas import tpu as pltpu
from jax.sharding import PartitionSpec as P

EPS = 1e-5
MESH = pl.DeviceIdType.MESH
ROWS = 32
WIDE = 256
CHUNK = 128
LAG = 4


def _kernel(x_hbm, g_ref, w1_hbm, w2_hbm, y_ref, w1v, w2v, inbuf, hbuf, acc, abuf, up0, up1, up2, over0, over1, over2,
            xsem, lsem, rsem, ssem, fsem, usem, ovsem, oss, dss, zrsem, zssem, *, S):
    s = lax.axis_index('stage')
    tp = lax.axis_index('tp')
    c = tp % 2
    sib = tp + 1 - 2 * c
    nbr = (tp + 2 - 4 * ((tp // 2) % 2), tp + 4 - 8 * (tp // 4))
    NB, _, _, D, U = w1v.shape
    R = inbuf.shape[0]
    LW = [(l, w) for w in range(3) for l in range(2)]
    H = U // 2
    up, over = (up0, up1, up2), (over0, over1, over2)

    def slot(b, j, k, w):
        if w == 0:
            return w1v.at[b, j, k]
        return w2v.at[b, j, pl.ds(pl.multiple_of(k * U + (w - 1) * H, H), H)]

    def load(b, q, w):
        src = w1_hbm.at[0, b, :, pl.ds(q * U, U)] if w == 0 else w2_hbm.at[0, b, pl.ds(q * U + (w - 1) * H, H)]
        return pltpu.make_async_copy(src, slot(b, 0, 2 * c + q, w), lsem.at[b, q, w])

    def remote(src, dst, ssem_, rsem_, stage, to):
        return pltpu.make_async_remote_copy(src_ref=src, dst_ref=dst, send_sem=ssem_, recv_sem=rsem_,
                                            device_id=(stage, to), device_id_type=MESH)

    def send(b, j, l, w):
        src = (slot(b, 0, 2 * c + l, w), slot(b, 0, 2 * c + 1 - l, w), slot(b, 1, 2 * c + 1 - l, w))[j - 1]
        return remote(src, slot(b, j, 2 * c + l, w), ssem.at[b, j - 1, l, w], rsem.at[b, j, 2 * c + l, w], s, nbr[l])

    def share(b, j, l, w):
        u = slot(b, j, 2 * c + l, w)
        return remote(u, u, fsem.at[b, j, l, w], rsem.at[b, j, 2 * c + l, w], s, sib)

    def arrived(b, j, k, w):
        u = slot(b, j, k, w)
        remote(u, u, fsem.at[b, j, 0, w], rsem.at[b, j, k, w], s, sib).wait_recv()

    def helped(w):
        return (s < S - 1) if w < 2 else (s == 1)

    def helper(w):
        return (s > 0) if w < 2 else (s == 2)

    def go_up(l, w):
        return remote(slot(1, 0, 2 * c + 1 - l, w), up[w].at[l], ssem.at[1, 1, l, w], usem.at[l, w], s + 1, tp)

    def go_over(l, w):
        return remote(up[w].at[l], over[w].at[l], oss.at[l, w], ovsem.at[l, w], s, nbr[l])

    def go_down(l, w):
        return remote(over[w].at[l], slot(1, 2, 2 * c + l, w), dss.at[l, w], rsem.at[1, 2, 2 * c + l, w], s - 1, tp)

    def each_part(cond, body):
        for w in range(3):
            @pl.when(cond(w))
            def _(w=w):
                for l in range(2):
                    body(l, w)

    def rows_of(i):
        return pl.ds(pl.multiple_of(i * CHUNK, CHUNK), CHUNK)

    def zsend(i):
        r = rows_of(i)
        return remote(y_ref.at[r], inbuf.at[r], zssem.at[i], zrsem.at[i], s + 1, tp)

    def each(n, body):
        def step(i, carry):
            body(i)
            return carry
        lax.fori_loop(0, n, step, 0)

    xin = pltpu.make_async_copy(x_hbm, inbuf, xsem)
    for b in range(NB):
        for q, w in LW:
            load(b, q, w).start()

    @pl.when(s == 0)
    def _():
        xin.start()

    barrier = pltpu.get_barrier_semaphore()
    for to in (sib, *nbr):
        pl.semaphore_signal(barrier, inc=1, device_id=(s, to), device_id_type=MESH)

    @pl.when(s > 0)
    def _():
        pl.semaphore_signal(barrier, inc=1, device_id=(s - 1, tp), device_id_type=MESH)

    @pl.when(s < S - 1)
    def _():
        pl.semaphore_signal(barrier, inc=1, device_id=(s + 1, tp), device_id_type=MESH)
    edge = (s == 0) | (s == S - 1)

    @pl.when(edge)
    def _():
        pl.semaphore_wait(barrier, 4)

    @pl.when(jnp.logical_not(edge))
    def _():
        pl.semaphore_wait(barrier, 5)

    for l, w in LW:
        load(0, l, w).wait()
    for j in (1, 2):
        for l, w in LW:
            send(0, j, l, w).start()
    for l, w in LW:
        load(1, l, w).wait()
    each_part(helped, lambda l, w: go_up(l, w).start())
    for b in range(NB):
        for l, w in LW:
            share(b, 0, l, w).start()

    def own_next():
        for l, w in LW:
            send(1, 1, l, w).start()

        each_part(lambda w: jnp.logical_not(helped(w)), lambda l, w: send(1, 2, l, w).start())

    def relay(b, j, on):
        for l, w in LW:
            arrived(b, j, 2 * c + l, w)
            if on:
                send(b, 3, 1 - l, w).start()
            share(b, j, l, w).start()

    def others(b, j):
        for l, w in LW:
            arrived(b, j, 2 * (1 - c) + l, w)

    def norm(r0, n, b, src):
        g = g_ref[0, pl.ds(b, 1), :].astype(jnp.float32)
        for r in range(0, n, ROWS):
            rows = pl.ds(r0 + r, ROWS)
            yf = src[rows, :].astype(jnp.bfloat16).astype(jnp.float32)
            acc[rows, :] = yf
            yc = yf - jnp.mean(yf, axis=-1, keepdims=True)
            var = jnp.mean(jnp.square(yc), axis=-1, keepdims=True)
            hbuf[rows, :] = (yc * lax.rsqrt(var + EPS) * g).astype(jnp.bfloat16)

    def mlp(rows, b, j0, steps):
        h = hbuf[rows, :]
        n = steps * 4 * U
        for i in range(steps):
            for k in range(4):
                z = jnp.dot(h, w1v[b, j0 + i, k], preferred_element_type=jnp.float32)
                abuf[:rows.size, (4 * i + k) * U:(4 * i + k + 1) * U] = jax.nn.gelu(z).astype(jnp.bfloat16)
        w2 = w2v[b, j0] if steps == 1 else w2v[b, j0:j0 + steps].reshape(n, D)
        acc[rows, :] += jnp.dot(abuf[:rows.size, :n], w2, preferred_element_type=jnp.float32)

    def finish(i):
        rows = rows_of(i)
        y_ref[rows, :] = acc[rows, :].astype(jnp.bfloat16)

    @pl.when(s == 0)
    def _():
        xin.wait()
        each(R // WIDE, lambda i: norm(pl.multiple_of(i * WIDE, WIDE), WIDE, 0, inbuf))

        def events(b, j):
            if j:
                relay(b, j, j == 1)
            if (b, j) == (0, 2):
                own_next()
            others(b, j)

        def step(t):
            b, j = t // 4, t % 4
            for e in range(4 * NB - 1):
                @pl.when(t == e)
                def _(e=e):
                    events(e // 4, e % 4)

            each(R // WIDE, lambda i: mlp(pl.ds(pl.multiple_of(i * WIDE, WIDE), WIDE), b, j, 1))

            @pl.when(t == 3)
            def _():
                each(R // WIDE, lambda i: norm(pl.multiple_of(i * WIDE, WIDE), WIDE, 1, acc))
        each(4 * NB - 1, step)
        events(NB - 1, 3)

        lag = LAG * c

        def last(i):
            mlp(rows_of(i), NB - 1, 3, 1)
            finish(i)

            @pl.when(i >= lag)
            def _():
                zsend(i - lag).start()
        each(R // CHUNK, last)

        @pl.when(c == 1)
        def _():
            each(LAG, lambda i: zsend(R // CHUNK - LAG + i).start())

    @pl.when(s > 0)
    def _():
        relay(0, 1, False)
        def over_(l, w):
            go_up(l, w).wait_recv()
            go_over(l, w).start()

        def down_(l, w):
            go_over(l, w).wait_recv()
            go_down(l, w).start()
        each_part(helper, over_)
        for l, w in LW:
            send(0, 3, l, w).start()
        relay(0, 2, False)
        own_next()
        each_part(helper, down_)
        relay(0, 3, False)
        relay(1, 1, True)
        relay(1, 2, False)
        relay(1, 3, False)
        for b in range(NB):
            for j in range(4):
                others(b, j)

        def body(i):
            zsend(i).wait_recv()
            rows = rows_of(i)
            for b in range(NB):
                norm(rows.start, CHUNK, b, inbuf if b == 0 else acc)
                mlp(rows, b, 0, 4)
            finish(i)

            @pl.when(s < S - 1)
            def _():
                zsend(i).start()
        each(R // CHUNK, body)

    for b in range(NB):
        for j in range(4):
            for l, w in LW:
                share(b, j, l, w).wait_send()
                if j:
                    send(b, j, l, w).wait_send()

    def helped_on(l, w):
        go_over(l, w).wait_send()
        go_down(l, w).wait_send()
    each_part(helper, helped_on)

    @pl.when(s < S - 1)
    def _():
        each(R // CHUNK, lambda i: zsend(i).wait_send())


def solution(mesh):
    S = mesh.shape['stage']

    def local(x, g, w1, w2):
        M, T, D = x.shape
        R = M * T
        n = R // CHUNK
        NB, F = w1.shape[1], w1.shape[3]
        U = F // 2
        bf, f32 = jnp.bfloat16, jnp.float32
        dma = pltpu.SemaphoreType.DMA
        y = pl.pallas_call(
            functools.partial(_kernel, S=S),
            out_shape=pltpu.VMEM((R, D), bf),
            in_specs=[pl.BlockSpec(memory_space=pl.ANY), pl.BlockSpec(memory_space=pltpu.VMEM),
                      pl.BlockSpec(memory_space=pl.ANY), pl.BlockSpec(memory_space=pl.ANY)],
            out_specs=pl.BlockSpec(memory_space=pltpu.VMEM),
            scratch_shapes=[
                pltpu.VMEM((NB, 4, 4, D, U), bf), pltpu.VMEM((NB, 4, 4 * U, D), bf),
                pltpu.VMEM((R, D), bf), pltpu.VMEM((R, D), bf),
                pltpu.VMEM((R, D), f32), pltpu.VMEM((WIDE, 16 * U), bf),
                *([pltpu.VMEM((2, D, U), bf)] + [pltpu.VMEM((2, U // 2, D), bf)] * 2) * 2,
                dma(()), dma((NB, 2, 3)), dma((NB, 4, 4, 3)), dma((NB, 3, 2, 3)), dma((NB, 4, 2, 3)),
                dma((2, 3)), dma((2, 3)), dma((2, 3)), dma((2, 3)),
                dma((n,)), dma((n,)),
            ],
            compiler_params=pltpu.CompilerParams(
                collective_id=0, has_side_effects=True, vmem_limit_bytes=62 * 1000 * 1000),
        )(x.reshape(R, D), g, w1, w2)
        return y.reshape(1, M, T, D)

    return jax.shard_map(
        local, mesh=mesh,
        in_specs=(P(None, 'tp', None), P('stage', None, None),
                  P('stage', None, None, 'tp'), P('stage', None, 'tp', None)),
        out_specs=P('stage', None, 'tp', None), check_vma=False)
```

```python
import functools

import jax
import jax.numpy as jnp
from jax import lax
from jax.experimental import pallas as pl
from jax.experimental.pallas import tpu as pltpu
from jax.sharding import PartitionSpec as P

EPS = 1e-5
MESH = pl.DeviceIdType.MESH
ROWS = 32
WIDE = 256
CHUNK = 128
LAG = 4


def _kernel(x_hbm, g_ref, w1_hbm, w2_hbm, y_ref, w1v, w2v, inbuf, hbuf, acc, abuf, up0, up1, up2, over0, over1, over2,
            xsem, lsem, rsem, ssem, fsem, usem, ovsem, oss, dss, zrsem, zssem, *, S):
    s = lax.axis_index('stage')
    tp = lax.axis_index('tp')
    c = tp % 2
    sib = tp + 1 - 2 * c
    nbr = (tp + 2 - 4 * ((tp // 2) % 2), tp + 4 - 8 * (tp // 4))
    NB, _, _, D, U = w1v.shape
    R = inbuf.shape[0]
    LW = [(l, w) for w in range(3) for l in range(2)]
    H = U // 2
    up, over = (up0, up1, up2), (over0, over1, over2)

    def slot(b, j, k, w):
        if w == 0:
            return w1v.at[b, j, k]
        return w2v.at[b, j, pl.ds(pl.multiple_of(k * U + (w - 1) * H, H), H)]

    def load(b, q, w):
        src = w1_hbm.at[0, b, :, pl.ds(q * U, U)] if w == 0 else w2_hbm.at[0, b, pl.ds(q * U + (w - 1) * H, H)]
        return pltpu.make_async_copy(src, slot(b, 0, 2 * c + q, w), lsem.at[b, q, w])

    def remote(src, dst, ssem_, rsem_, stage, to):
        return pltpu.make_async_remote_copy(src_ref=src, dst_ref=dst, send_sem=ssem_, recv_sem=rsem_,
                                            device_id=(stage, to), device_id_type=MESH)

    def send(b, j, l, w):
        src = (slot(b, 0, 2 * c + l, w), slot(b, 0, 2 * c + 1 - l, w), slot(b, 1, 2 * c + 1 - l, w))[j - 1]
        return remote(src, slot(b, j, 2 * c + l, w), ssem.at[b, j - 1, l, w], rsem.at[b, j, 2 * c + l, w], s, nbr[l])

    def share(b, j, l, w):
        u = slot(b, j, 2 * c + l, w)
        return remote(u, u, fsem.at[b, j, l, w], rsem.at[b, j, 2 * c + l, w], s, sib)

    def arrived(b, j, k, w):
        u = slot(b, j, k, w)
        remote(u, u, fsem.at[b, j, 0, w], rsem.at[b, j, k, w], s, sib).wait_recv()

    def helped(w):
        return (s < S - 1) if w < 2 else (s == 1)

    def helper(w):
        return (s > 0) if w < 2 else (s == 2)

    def go_up(l, w):
        return remote(slot(1, 0, 2 * c + 1 - l, w), up[w].at[l], ssem.at[1, 1, l, w], usem.at[l, w], s + 1, tp)

    def go_over(l, w):
        return remote(up[w].at[l], over[w].at[l], oss.at[l, w], ovsem.at[l, w], s, nbr[l])

    def go_down(l, w):
        return remote(over[w].at[l], slot(1, 2, 2 * c + l, w), dss.at[l, w], rsem.at[1, 2, 2 * c + l, w], s - 1, tp)

    def each_part(cond, body):
        for w in range(3):
            @pl.when(cond(w))
            def _(w=w):
                for l in range(2):
                    body(l, w)

    def rows_of(i):
        return pl.ds(pl.multiple_of(i * CHUNK, CHUNK), CHUNK)

    def zsend(i):
        r = rows_of(i)
        return remote(y_ref.at[r], inbuf.at[r], zssem.at[i], zrsem.at[i], s + 1, tp)

    def each(n, body):
        def step(i, carry):
            body(i)
            return carry
        lax.fori_loop(0, n, step, 0)

    xin = pltpu.make_async_copy(x_hbm, inbuf, xsem)
    for b in range(NB):
        for q, w in LW:
            load(b, q, w).start()

    @pl.when(s == 0)
    def _():
        xin.start()

    barrier = pltpu.get_barrier_semaphore()
    for to in (sib, *nbr):
        pl.semaphore_signal(barrier, inc=1, device_id=(s, to), device_id_type=MESH)

    @pl.when(s > 0)
    def _():
        pl.semaphore_signal(barrier, inc=1, device_id=(s - 1, tp), device_id_type=MESH)

    @pl.when(s < S - 1)
    def _():
        pl.semaphore_signal(barrier, inc=1, device_id=(s + 1, tp), device_id_type=MESH)
    edge = (s == 0) | (s == S - 1)

    @pl.when(edge)
    def _():
        pl.semaphore_wait(barrier, 4)

    @pl.when(jnp.logical_not(edge))
    def _():
        pl.semaphore_wait(barrier, 5)

    for l, w in LW:
        load(0, l, w).wait()
    for j in (1, 2):
        for l, w in LW:
            send(0, j, l, w).start()
    for l, w in LW:
        load(1, l, w).wait()
    each_part(helped, lambda l, w: go_up(l, w).start())
    for b in range(NB):
        for l, w in LW:
            share(b, 0, l, w).start()

    def own_next():
        for l, w in LW:
            send(1, 1, l, w).start()

        each_part(lambda w: jnp.logical_not(helped(w)), lambda l, w: send(1, 2, l, w).start())

    def relay(b, j, on):
        for l, w in LW:
            arrived(b, j, 2 * c + l, w)
            if on:
                send(b, 3, 1 - l, w).start()
            share(b, j, l, w).start()
            if (b, j, l, w) == (0, 3, 1, 0):
                own_next()

    def others(b, j):
        for l, w in LW:
            arrived(b, j, 2 * (1 - c) + l, w)

    def norm(r0, n, b, src):
        g = g_ref[0, pl.ds(b, 1), :].astype(jnp.float32)
        for r in range(0, n, ROWS):
            rows = pl.ds(r0 + r, ROWS)
            yf = src[rows, :].astype(jnp.bfloat16).astype(jnp.float32)
            acc[rows, :] = yf
            yc = yf - jnp.mean(yf, axis=-1, keepdims=True)
            var = jnp.mean(jnp.square(yc), axis=-1, keepdims=True)
            hbuf[rows, :] = (yc * lax.rsqrt(var + EPS) * g).astype(jnp.bfloat16)

    def mlp(rows, b, j0, steps):
        h = hbuf[rows, :]
        n = steps * 4 * U
        for i in range(steps):
            for k in range(4):
                z = jnp.dot(h, w1v[b, j0 + i, k], preferred_element_type=jnp.float32)
                abuf[:rows.size, (4 * i + k) * U:(4 * i + k + 1) * U] = jax.nn.gelu(z).astype(jnp.bfloat16)
        w2 = w2v[b, j0] if steps == 1 else w2v[b, j0:j0 + steps].reshape(n, D)
        acc[rows, :] += jnp.dot(abuf[:rows.size, :n], w2, preferred_element_type=jnp.float32)

    def finish(i):
        rows = rows_of(i)
        y_ref[rows, :] = acc[rows, :].astype(jnp.bfloat16)

    @pl.when(s == 0)
    def _():
        xin.wait()
        each(R // WIDE, lambda i: norm(pl.multiple_of(i * WIDE, WIDE), WIDE, 0, inbuf))

        def events(b, j):
            if j:
                relay(b, j, j == 1)
            others(b, j)

        def step(t):
            b, j = t // 4, t % 4
            for e in range(4 * NB - 1):
                @pl.when(t == e)
                def _(e=e):
                    events(e // 4, e % 4)

            each(R // WIDE, lambda i: mlp(pl.ds(pl.multiple_of(i * WIDE, WIDE), WIDE), b, j, 1))

            @pl.when(t == 3)
            def _():
                each(R // WIDE, lambda i: norm(pl.multiple_of(i * WIDE, WIDE), WIDE, 1, acc))
        each(4 * NB - 1, step)
        events(NB - 1, 3)

        lag = LAG * c

        def last(i):
            mlp(rows_of(i), NB - 1, 3, 1)
            finish(i)

            @pl.when(i >= lag)
            def _():
                zsend(i - lag).start()
        each(R // CHUNK, last)

        @pl.when(c == 1)
        def _():
            each(LAG, lambda i: zsend(R // CHUNK - LAG + i).start())

    @pl.when(s > 0)
    def _():
        relay(0, 1, False)
        def over_(l, w):
            go_up(l, w).wait_recv()
            go_over(l, w).start()

        def down_(l, w):
            go_over(l, w).wait_recv()
            go_down(l, w).start()
        each_part(helper, over_)
        for l, w in LW:
            send(0, 3, l, w).start()
        relay(0, 2, False)
        each_part(helper, down_)
        relay(0, 3, False)
        relay(1, 1, True)
        relay(1, 2, False)
        relay(1, 3, False)
        for b in range(NB):
            for j in range(4):
                others(b, j)

        def body(i):
            zsend(i).wait_recv()
            rows = rows_of(i)
            for b in range(NB):
                norm(rows.start, CHUNK, b, inbuf if b == 0 else acc)
                mlp(rows, b, 0, 4)
            finish(i)

            @pl.when(s < S - 1)
            def _():
                zsend(i).start()
        each(R // CHUNK, body)

    for b in range(NB):
        for j in range(4):
            for l, w in LW:
                share(b, j, l, w).wait_send()
                if j:
                    send(b, j, l, w).wait_send()

    def helped_on(l, w):
        go_over(l, w).wait_send()
        go_down(l, w).wait_send()
    each_part(helper, helped_on)

    @pl.when(s < S - 1)
    def _():
        each(R // CHUNK, lambda i: zsend(i).wait_send())


def solution(mesh):
    S = mesh.shape['stage']

    def local(x, g, w1, w2):
        M, T, D = x.shape
        R = M * T
        n = R // CHUNK
        NB, F = w1.shape[1], w1.shape[3]
        U = F // 2
        bf, f32 = jnp.bfloat16, jnp.float32
        dma = pltpu.SemaphoreType.DMA
        y = pl.pallas_call(
            functools.partial(_kernel, S=S),
            out_shape=pltpu.VMEM((R, D), bf),
            in_specs=[pl.BlockSpec(memory_space=pl.ANY), pl.BlockSpec(memory_space=pltpu.VMEM),
                      pl.BlockSpec(memory_space=pl.ANY), pl.BlockSpec(memory_space=pl.ANY)],
            out_specs=pl.BlockSpec(memory_space=pltpu.VMEM),
            scratch_shapes=[
                pltpu.VMEM((NB, 4, 4, D, U), bf), pltpu.VMEM((NB, 4, 4 * U, D), bf),
                pltpu.VMEM((R, D), bf), pltpu.VMEM((R, D), bf),
                pltpu.VMEM((R, D), f32), pltpu.VMEM((WIDE, 16 * U), bf),
                *([pltpu.VMEM((2, D, U), bf)] + [pltpu.VMEM((2, U // 2, D), bf)] * 2) * 2,
                dma(()), dma((NB, 2, 3)), dma((NB, 4, 4, 3)), dma((NB, 3, 2, 3)), dma((NB, 4, 2, 3)),
                dma((2, 3)), dma((2, 3)), dma((2, 3)), dma((2, 3)),
                dma((n,)), dma((n,)),
            ],
            compiler_params=pltpu.CompilerParams(
                collective_id=0, has_side_effects=True, vmem_limit_bytes=62 * 1000 * 1000),
        )(x.reshape(R, D), g, w1, w2)
        return y.reshape(1, M, T, D)

    return jax.shard_map(
        local, mesh=mesh,
        in_specs=(P(None, 'tp', None), P('stage', None, None),
                  P('stage', None, None, 'tp'), P('stage', None, 'tp', None)),
        out_specs=P('stage', None, 'tp', None), check_vma=False)
```

```python
import functools

import jax
import jax.numpy as jnp
from jax import lax
from jax.experimental import pallas as pl
from jax.experimental.pallas import tpu as pltpu
from jax.sharding import PartitionSpec as P

EPS = 1e-5
MESH = pl.DeviceIdType.MESH
ROWS = 32
WIDE = 256
CHUNK = 128
LAG = 4


def _kernel(x_hbm, g_ref, w1_hbm, w2_hbm, y_ref, w1v, w2v, inbuf, hbuf, acc, abuf, up0, up1, up2, over0, over1, over2,
            xsem, lsem, rsem, ssem, fsem, usem, ovsem, oss, dss, zrsem, zssem, *, S):
    s = lax.axis_index('stage')
    tp = lax.axis_index('tp')
    c = tp % 2
    sib = tp + 1 - 2 * c
    nbr = (tp + 2 - 4 * ((tp // 2) % 2), tp + 4 - 8 * (tp // 4))
    NB, _, _, D, U = w1v.shape
    R = inbuf.shape[0]
    LW = [(l, w) for w in range(3) for l in range(2)]
    H = U // 2
    up, over = (up0, up1, up2), (over0, over1, over2)

    def slot(b, j, k, w):
        if w == 0:
            return w1v.at[b, j, k]
        return w2v.at[b, j, pl.ds(pl.multiple_of(k * U + (w - 1) * H, H), H)]

    def load(b, q, w):
        src = w1_hbm.at[0, b, :, pl.ds(q * U, U)] if w == 0 else w2_hbm.at[0, b, pl.ds(q * U + (w - 1) * H, H)]
        return pltpu.make_async_copy(src, slot(b, 0, 2 * c + q, w), lsem.at[b, q, w])

    def remote(src, dst, ssem_, rsem_, stage, to):
        return pltpu.make_async_remote_copy(src_ref=src, dst_ref=dst, send_sem=ssem_, recv_sem=rsem_,
                                            device_id=(stage, to), device_id_type=MESH)

    def send(b, j, l, w):
        src = (slot(b, 0, 2 * c + l, w), slot(b, 0, 2 * c + 1 - l, w), slot(b, 1, 2 * c + 1 - l, w))[j - 1]
        return remote(src, slot(b, j, 2 * c + l, w), ssem.at[b, j - 1, l, w], rsem.at[b, j, 2 * c + l, w], s, nbr[l])

    def share(b, j, l, w):
        u = slot(b, j, 2 * c + l, w)
        return remote(u, u, fsem.at[b, j, l, w], rsem.at[b, j, 2 * c + l, w], s, sib)

    def arrived(b, j, k, w):
        u = slot(b, j, k, w)
        remote(u, u, fsem.at[b, j, 0, w], rsem.at[b, j, k, w], s, sib).wait_recv()

    def helped(w):
        return (s < S - 1) if w < 2 else (s == 1)

    def helper(w):
        return (s > 0) if w < 2 else (s == 2)

    def go_up(l, w):
        return remote(slot(1, 0, 2 * c + 1 - l, w), up[w].at[l], ssem.at[1, 1, l, w], usem.at[l, w], s + 1, tp)

    def go_over(l, w):
        return remote(up[w].at[l], over[w].at[l], oss.at[l, w], ovsem.at[l, w], s, nbr[l])

    def go_down(l, w):
        return remote(over[w].at[l], slot(1, 2, 2 * c + l, w), dss.at[l, w], rsem.at[1, 2, 2 * c + l, w], s - 1, tp)

    def each_part(cond, body):
        for w in range(3):
            @pl.when(cond(w))
            def _(w=w):
                for l in range(2):
                    body(l, w)

    def rows_of(i):
        return pl.ds(pl.multiple_of(i * CHUNK, CHUNK), CHUNK)

    def zsend(i):
        r = rows_of(i)
        return remote(y_ref.at[r], inbuf.at[r], zssem.at[i], zrsem.at[i], s + 1, tp)

    def each(n, body):
        def step(i, carry):
            body(i)
            return carry
        lax.fori_loop(0, n, step, 0)

    xin = pltpu.make_async_copy(x_hbm, inbuf, xsem)
    for b in range(NB):
        for q, w in LW:
            load(b, q, w).start()

    @pl.when(s == 0)
    def _():
        xin.start()

    barrier = pltpu.get_barrier_semaphore()
    for to in (sib, *nbr):
        pl.semaphore_signal(barrier, inc=1, device_id=(s, to), device_id_type=MESH)

    @pl.when(s > 0)
    def _():
        pl.semaphore_signal(barrier, inc=1, device_id=(s - 1, tp), device_id_type=MESH)

    @pl.when(s < S - 1)
    def _():
        pl.semaphore_signal(barrier, inc=1, device_id=(s + 1, tp), device_id_type=MESH)
    edge = (s == 0) | (s == S - 1)

    @pl.when(edge)
    def _():
        pl.semaphore_wait(barrier, 4)

    @pl.when(jnp.logical_not(edge))
    def _():
        pl.semaphore_wait(barrier, 5)

    for l, w in LW:
        load(0, l, w).wait()
    for j in (1, 2):
        for l, w in LW:
            send(0, j, l, w).start()
    for l, w in LW:
        load(1, l, w).wait()
    each_part(helped, lambda l, w: go_up(l, w).start())
    for b in range(NB):
        for l, w in LW:
            share(b, 0, l, w).start()

    def own_next():
        for l, w in LW:
            send(1, 1, l, w).start()

        each_part(lambda w: jnp.logical_not(helped(w)), lambda l, w: send(1, 2, l, w).start())

    def relay(b, j, on):
        for l, w in LW:
            arrived(b, j, 2 * c + l, w)
            if on:
                send(b, 3, 1 - l, w).start()
            share(b, j, l, w).start()
            if (b, j, l, w) == (0, 3, 1, 0):
                own_next()

    def others(b, j):
        for l, w in LW:
            arrived(b, j, 2 * (1 - c) + l, w)

    def norm(r0, n, b, src):
        g = g_ref[0, pl.ds(b, 1), :].astype(jnp.float32)
        for r in range(0, n, ROWS):
            rows = pl.ds(r0 + r, ROWS)
            yf = src[rows, :].astype(jnp.bfloat16).astype(jnp.float32)
            acc[rows, :] = yf
            yc = yf - jnp.mean(yf, axis=-1, keepdims=True)
            var = jnp.mean(jnp.square(yc), axis=-1, keepdims=True)
            hbuf[rows, :] = (yc * lax.rsqrt(var + EPS) * g).astype(jnp.bfloat16)

    def mlp(rows, b, j0, steps):
        h = hbuf[rows, :]
        n = steps * 4 * U
        for i in range(steps):
            for k in range(4):
                z = jnp.dot(h, w1v[b, j0 + i, k], preferred_element_type=jnp.float32)
                abuf[:rows.size, (4 * i + k) * U:(4 * i + k + 1) * U] = jax.nn.gelu(z).astype(jnp.bfloat16)
        w2 = w2v[b, j0] if steps == 1 else w2v[b, j0:j0 + steps].reshape(n, D)
        acc[rows, :] += jnp.dot(abuf[:rows.size, :n], w2, preferred_element_type=jnp.float32)

    def finish(i):
        rows = rows_of(i)
        y_ref[rows, :] = acc[rows, :].astype(jnp.bfloat16)

    @pl.when(s == 0)
    def _():
        xin.wait()
        each(R // WIDE, lambda i: norm(pl.multiple_of(i * WIDE, WIDE), WIDE, 0, inbuf))

        def events(b, j):
            if j and (b, j) != (1, 1):
                relay(b, j, j == 1)
            others(b, j)

        def step(t):
            b, j = t // 4, t % 4
            for e in range(4 * NB - 1):
                @pl.when(t == e)
                def _(e=e):
                    events(e // 4, e % 4)

            def wide(i):
                @pl.when((t == 4) & (i == R // WIDE // 2))
                def _():
                    relay(1, 1, True)
                mlp(pl.ds(pl.multiple_of(i * WIDE, WIDE), WIDE), b, j, 1)
            each(R // WIDE, wide)

            @pl.when(t == 3)
            def _():
                each(R // WIDE, lambda i: norm(pl.multiple_of(i * WIDE, WIDE), WIDE, 1, acc))
        each(4 * NB - 1, step)
        events(NB - 1, 3)

        lag = LAG * c

        def last(i):
            mlp(rows_of(i), NB - 1, 3, 1)
            finish(i)

            @pl.when(i >= lag)
            def _():
                zsend(i - lag).start()
        each(R // CHUNK, last)

        @pl.when(c == 1)
        def _():
            each(LAG, lambda i: zsend(R // CHUNK - LAG + i).start())

    @pl.when(s > 0)
    def _():
        relay(0, 1, False)
        def over_(l, w):
            go_up(l, w).wait_recv()
            go_over(l, w).start()

        def down_(l, w):
            go_over(l, w).wait_recv()
            go_down(l, w).start()
        each_part(helper, over_)
        for l, w in LW:
            send(0, 3, l, w).start()
        relay(0, 2, False)
        each_part(helper, down_)
        relay(0, 3, False)
        relay(1, 1, True)
        relay(1, 2, False)
        relay(1, 3, False)
        for b in range(NB):
            for j in range(4):
                others(b, j)

        def body(i):
            zsend(i).wait_recv()
            rows = rows_of(i)
            for b in range(NB):
                norm(rows.start, CHUNK, b, inbuf if b == 0 else acc)
                mlp(rows, b, 0, 4)
            finish(i)

            @pl.when(s < S - 1)
            def _():
                zsend(i).start()
        each(R // CHUNK, body)

    for b in range(NB):
        for j in range(4):
            for l, w in LW:
                share(b, j, l, w).wait_send()
                if j:
                    send(b, j, l, w).wait_send()

    def helped_on(l, w):
        go_over(l, w).wait_send()
        go_down(l, w).wait_send()
    each_part(helper, helped_on)

    @pl.when(s < S - 1)
    def _():
        each(R // CHUNK, lambda i: zsend(i).wait_send())


def solution(mesh):
    S = mesh.shape['stage']

    def local(x, g, w1, w2):
        M, T, D = x.shape
        R = M * T
        n = R // CHUNK
        NB, F = w1.shape[1], w1.shape[3]
        U = F // 2
        bf, f32 = jnp.bfloat16, jnp.float32
        dma = pltpu.SemaphoreType.DMA
        y = pl.pallas_call(
            functools.partial(_kernel, S=S),
            out_shape=pltpu.VMEM((R, D), bf),
            in_specs=[pl.BlockSpec(memory_space=pl.ANY), pl.BlockSpec(memory_space=pltpu.VMEM),
                      pl.BlockSpec(memory_space=pl.ANY), pl.BlockSpec(memory_space=pl.ANY)],
            out_specs=pl.BlockSpec(memory_space=pltpu.VMEM),
            scratch_shapes=[
                pltpu.VMEM((NB, 4, 4, D, U), bf), pltpu.VMEM((NB, 4, 4 * U, D), bf),
                pltpu.VMEM((R, D), bf), pltpu.VMEM((R, D), bf),
                pltpu.VMEM((R, D), f32), pltpu.VMEM((WIDE, 16 * U), bf),
                *([pltpu.VMEM((2, D, U), bf)] + [pltpu.VMEM((2, U // 2, D), bf)] * 2) * 2,
                dma(()), dma((NB, 2, 3)), dma((NB, 4, 4, 3)), dma((NB, 3, 2, 3)), dma((NB, 4, 2, 3)),
                dma((2, 3)), dma((2, 3)), dma((2, 3)), dma((2, 3)),
                dma((n,)), dma((n,)),
            ],
            compiler_params=pltpu.CompilerParams(
                collective_id=0, has_side_effects=True, vmem_limit_bytes=62 * 1000 * 1000),
        )(x.reshape(R, D), g, w1, w2)
        return y.reshape(1, M, T, D)

    return jax.shard_map(
        local, mesh=mesh,
        in_specs=(P(None, 'tp', None), P('stage', None, None),
                  P('stage', None, None, 'tp'), P('stage', None, 'tp', None)),
        out_specs=P('stage', None, 'tp', None), check_vma=False)
```

```python
import functools

import jax
import jax.numpy as jnp
from jax import lax
from jax.experimental import pallas as pl
from jax.experimental.pallas import tpu as pltpu
from jax.sharding import PartitionSpec as P

EPS = 1e-5
MESH = pl.DeviceIdType.MESH
ROWS = 32
WIDE = 256
CHUNK = 128
LAG = 2


def _kernel(x_hbm, g_ref, w1_hbm, w2_hbm, y_ref, w1v, w2v, inbuf, hbuf, acc, abuf, up0, up1, up2, over0, over1, over2,
            xsem, lsem, rsem, ssem, fsem, usem, ovsem, oss, dss, zrsem, zssem, *, S):
    s = lax.axis_index('stage')
    tp = lax.axis_index('tp')
    c = tp % 2
    sib = tp + 1 - 2 * c
    nbr = (tp + 2 - 4 * ((tp // 2) % 2), tp + 4 - 8 * (tp // 4))
    NB, _, _, D, U = w1v.shape
    R = inbuf.shape[0]
    LW = [(l, w) for w in range(3) for l in range(2)]
    H = U // 2
    up, over = (up0, up1, up2), (over0, over1, over2)

    def slot(b, j, k, w):
        if w == 0:
            return w1v.at[b, j, k]
        return w2v.at[b, j, pl.ds(pl.multiple_of(k * U + (w - 1) * H, H), H)]

    def load(b, q, w):
        src = w1_hbm.at[0, b, :, pl.ds(q * U, U)] if w == 0 else w2_hbm.at[0, b, pl.ds(q * U + (w - 1) * H, H)]
        return pltpu.make_async_copy(src, slot(b, 0, 2 * c + q, w), lsem.at[b, q, w])

    def remote(src, dst, ssem_, rsem_, stage, to):
        return pltpu.make_async_remote_copy(src_ref=src, dst_ref=dst, send_sem=ssem_, recv_sem=rsem_,
                                            device_id=(stage, to), device_id_type=MESH)

    def send(b, j, l, w):
        src = (slot(b, 0, 2 * c + l, w), slot(b, 0, 2 * c + 1 - l, w), slot(b, 1, 2 * c + 1 - l, w))[j - 1]
        return remote(src, slot(b, j, 2 * c + l, w), ssem.at[b, j - 1, l, w], rsem.at[b, j, 2 * c + l, w], s, nbr[l])

    def share(b, j, l, w):
        u = slot(b, j, 2 * c + l, w)
        return remote(u, u, fsem.at[b, j, l, w], rsem.at[b, j, 2 * c + l, w], s, sib)

    def arrived(b, j, k, w):
        u = slot(b, j, k, w)
        remote(u, u, fsem.at[b, j, 0, w], rsem.at[b, j, k, w], s, sib).wait_recv()

    def helped(w):
        return (s < S - 1) if w < 2 else (s == 1)

    def helper(w):
        return (s > 0) if w < 2 else (s == 2)

    def go_up(l, w):
        return remote(slot(1, 0, 2 * c + 1 - l, w), up[w].at[l], ssem.at[1, 1, l, w], usem.at[l, w], s + 1, tp)

    def go_over(l, w):
        return remote(up[w].at[l], over[w].at[l], oss.at[l, w], ovsem.at[l, w], s, nbr[l])

    def go_down(l, w):
        return remote(over[w].at[l], slot(1, 2, 2 * c + l, w), dss.at[l, w], rsem.at[1, 2, 2 * c + l, w], s - 1, tp)

    def each_part(cond, body):
        for w in range(3):
            @pl.when(cond(w))
            def _(w=w):
                for l in range(2):
                    body(l, w)

    def rows_of(i):
        return pl.ds(pl.multiple_of(i * CHUNK, CHUNK), CHUNK)

    def zsend(i):
        r = rows_of(i)
        return remote(y_ref.at[r], inbuf.at[r], zssem.at[i], zrsem.at[i], s + 1, tp)

    def each(n, body):
        def step(i, carry):
            body(i)
            return carry
        lax.fori_loop(0, n, step, 0)

    xin = pltpu.make_async_copy(x_hbm, inbuf, xsem)
    for b in range(NB):
        for q, w in LW:
            load(b, q, w).start()

    @pl.when(s == 0)
    def _():
        xin.start()

    barrier = pltpu.get_barrier_semaphore()
    for to in (sib, *nbr):
        pl.semaphore_signal(barrier, inc=1, device_id=(s, to), device_id_type=MESH)

    @pl.when(s > 0)
    def _():
        pl.semaphore_signal(barrier, inc=1, device_id=(s - 1, tp), device_id_type=MESH)

    @pl.when(s < S - 1)
    def _():
        pl.semaphore_signal(barrier, inc=1, device_id=(s + 1, tp), device_id_type=MESH)
    edge = (s == 0) | (s == S - 1)

    @pl.when(edge)
    def _():
        pl.semaphore_wait(barrier, 4)

    @pl.when(jnp.logical_not(edge))
    def _():
        pl.semaphore_wait(barrier, 5)

    for l, w in LW:
        load(0, l, w).wait()
    for j in (1, 2):
        for l, w in LW:
            send(0, j, l, w).start()
    for l, w in LW:
        load(1, l, w).wait()
    each_part(helped, lambda l, w: go_up(l, w).start())
    for b in range(NB):
        for l, w in LW:
            share(b, 0, l, w).start()

    def own_next():
        for l, w in LW:
            send(1, 1, l, w).start()

        each_part(lambda w: jnp.logical_not(helped(w)), lambda l, w: send(1, 2, l, w).start())

    def relay(b, j, on):
        for l, w in LW:
            arrived(b, j, 2 * c + l, w)
            if on:
                send(b, 3, 1 - l, w).start()
            share(b, j, l, w).start()
            if (b, j, l, w) == (0, 3, 1, 0):
                own_next()

    def others(b, j):
        for l, w in LW:
            arrived(b, j, 2 * (1 - c) + l, w)

    def norm(r0, n, b, src):
        g = g_ref[0, pl.ds(b, 1), :].astype(jnp.float32)
        for r in range(0, n, ROWS):
            rows = pl.ds(r0 + r, ROWS)
            yf = src[rows, :].astype(jnp.bfloat16).astype(jnp.float32)
            acc[rows, :] = yf
            yc = yf - jnp.mean(yf, axis=-1, keepdims=True)
            var = jnp.mean(jnp.square(yc), axis=-1, keepdims=True)
            hbuf[rows, :] = (yc * lax.rsqrt(var + EPS) * g).astype(jnp.bfloat16)

    def mlp(rows, b, j0, steps):
        h = hbuf[rows, :]
        n = steps * 4 * U
        for i in range(steps):
            for k in range(4):
                z = jnp.dot(h, w1v[b, j0 + i, k], preferred_element_type=jnp.float32)
                abuf[:rows.size, (4 * i + k) * U:(4 * i + k + 1) * U] = jax.nn.gelu(z).astype(jnp.bfloat16)
        w2 = w2v[b, j0] if steps == 1 else w2v[b, j0:j0 + steps].reshape(n, D)
        acc[rows, :] += jnp.dot(abuf[:rows.size, :n], w2, preferred_element_type=jnp.float32)

    def finish(i):
        rows = rows_of(i)
        y_ref[rows, :] = acc[rows, :].astype(jnp.bfloat16)

    @pl.when(s == 0)
    def _():
        xin.wait()
        each(R // WIDE, lambda i: norm(pl.multiple_of(i * WIDE, WIDE), WIDE, 0, inbuf))

        def events(b, j):
            if j and (b, j) != (1, 1):
                relay(b, j, j == 1)
            others(b, j)

        def step(t):
            b, j = t // 4, t % 4
            for e in range(4 * NB - 1):
                @pl.when(t == e)
                def _(e=e):
                    events(e // 4, e % 4)

            def wide(i):
                @pl.when((t == 4) & (i == R // WIDE // 2))
                def _():
                    relay(1, 1, True)
                mlp(pl.ds(pl.multiple_of(i * WIDE, WIDE), WIDE), b, j, 1)
            each(R // WIDE, wide)

            @pl.when(t == 3)
            def _():
                each(R // WIDE, lambda i: norm(pl.multiple_of(i * WIDE, WIDE), WIDE, 1, acc))
        each(4 * NB - 1, step)
        events(NB - 1, 3)

        lag = LAG * c

        def last(i):
            mlp(rows_of(i), NB - 1, 3, 1)
            finish(i)

            @pl.when(i >= lag)
            def _():
                zsend(i - lag).start()
        each(R // CHUNK, last)

        @pl.when(c == 1)
        def _():
            each(LAG, lambda i: zsend(R // CHUNK - LAG + i).start())

    @pl.when(s > 0)
    def _():
        relay(0, 1, False)
        def over_(l, w):
            go_up(l, w).wait_recv()
            go_over(l, w).start()

        def down_(l, w):
            go_over(l, w).wait_recv()
            go_down(l, w).start()
        each_part(helper, over_)
        for l, w in LW:
            send(0, 3, l, w).start()
        relay(0, 2, False)
        each_part(helper, down_)
        relay(0, 3, False)
        relay(1, 1, True)
        relay(1, 2, False)
        relay(1, 3, False)
        for b in range(NB):
            for j in range(4):
                others(b, j)

        def body(i):
            zsend(i).wait_recv()
            rows = rows_of(i)
            for b in range(NB):
                norm(rows.start, CHUNK, b, inbuf if b == 0 else acc)
                mlp(rows, b, 0, 4)
            finish(i)

            @pl.when(s < S - 1)
            def _():
                zsend(i).start()
        each(R // CHUNK, body)

    for b in range(NB):
        for j in range(4):
            for l, w in LW:
                share(b, j, l, w).wait_send()
                if j:
                    send(b, j, l, w).wait_send()

    def helped_on(l, w):
        go_over(l, w).wait_send()
        go_down(l, w).wait_send()
    each_part(helper, helped_on)

    @pl.when(s < S - 1)
    def _():
        each(R // CHUNK, lambda i: zsend(i).wait_send())


def solution(mesh):
    S = mesh.shape['stage']

    def local(x, g, w1, w2):
        M, T, D = x.shape
        R = M * T
        n = R // CHUNK
        NB, F = w1.shape[1], w1.shape[3]
        U = F // 2
        bf, f32 = jnp.bfloat16, jnp.float32
        dma = pltpu.SemaphoreType.DMA
        y = pl.pallas_call(
            functools.partial(_kernel, S=S),
            out_shape=pltpu.VMEM((R, D), bf),
            in_specs=[pl.BlockSpec(memory_space=pl.ANY), pl.BlockSpec(memory_space=pltpu.VMEM),
                      pl.BlockSpec(memory_space=pl.ANY), pl.BlockSpec(memory_space=pl.ANY)],
            out_specs=pl.BlockSpec(memory_space=pltpu.VMEM),
            scratch_shapes=[
                pltpu.VMEM((NB, 4, 4, D, U), bf), pltpu.VMEM((NB, 4, 4 * U, D), bf),
                pltpu.VMEM((R, D), bf), pltpu.VMEM((R, D), bf),
                pltpu.VMEM((R, D), f32), pltpu.VMEM((WIDE, 16 * U), bf),
                *([pltpu.VMEM((2, D, U), bf)] + [pltpu.VMEM((2, U // 2, D), bf)] * 2) * 2,
                dma(()), dma((NB, 2, 3)), dma((NB, 4, 4, 3)), dma((NB, 3, 2, 3)), dma((NB, 4, 2, 3)),
                dma((2, 3)), dma((2, 3)), dma((2, 3)), dma((2, 3)),
                dma((n,)), dma((n,)),
            ],
            compiler_params=pltpu.CompilerParams(
                collective_id=0, has_side_effects=True, vmem_limit_bytes=62 * 1000 * 1000),
        )(x.reshape(R, D), g, w1, w2)
        return y.reshape(1, M, T, D)

    return jax.shard_map(
        local, mesh=mesh,
        in_specs=(P(None, 'tp', None), P('stage', None, None),
                  P('stage', None, None, 'tp'), P('stage', None, 'tp', None)),
        out_specs=P('stage', None, 'tp', None), check_vma=False)
```

```python
import functools

import jax
import jax.numpy as jnp
from jax import lax
from jax.experimental import pallas as pl
from jax.experimental.pallas import tpu as pltpu
from jax.sharding import PartitionSpec as P

EPS = 1e-5
MESH = pl.DeviceIdType.MESH
ROWS = 32
WIDE = 256
CHUNK = 128
LAG = 2


def _kernel(x_hbm, g_ref, w1_hbm, w2_hbm, y_ref, w1v, w2v, inbuf, hbuf, acc, abuf, up0, up1, up2, over0, over1, over2,
            xsem, lsem, rsem, ssem, fsem, usem, ovsem, oss, dss, zrsem, zssem, *, S):
    s = lax.axis_index('stage')
    tp = lax.axis_index('tp')
    c = tp % 2
    sib = tp + 1 - 2 * c
    nbr = (tp + 2 - 4 * ((tp // 2) % 2), tp + 4 - 8 * (tp // 4))
    NB, _, _, D, U = w1v.shape
    R = inbuf.shape[0]
    LW = [(l, w) for w in range(3) for l in range(2)]
    H = U // 2
    up, over = (up0, up1, up2), (over0, over1, over2)

    def slot(b, j, k, w):
        if w == 0:
            return w1v.at[b, j, k]
        return w2v.at[b, j, pl.ds(pl.multiple_of(k * U + (w - 1) * H, H), H)]

    def load(b, q, w):
        src = w1_hbm.at[0, b, :, pl.ds(q * U, U)] if w == 0 else w2_hbm.at[0, b, pl.ds(q * U + (w - 1) * H, H)]
        return pltpu.make_async_copy(src, slot(b, 0, 2 * c + q, w), lsem.at[b, q, w])

    def remote(src, dst, ssem_, rsem_, stage, to):
        return pltpu.make_async_remote_copy(src_ref=src, dst_ref=dst, send_sem=ssem_, recv_sem=rsem_,
                                            device_id=(stage, to), device_id_type=MESH)

    def send(b, j, l, w):
        src = (slot(b, 0, 2 * c + l, w), slot(b, 0, 2 * c + 1 - l, w), slot(b, 1, 2 * c + 1 - l, w))[j - 1]
        return remote(src, slot(b, j, 2 * c + l, w), ssem.at[b, j - 1, l, w], rsem.at[b, j, 2 * c + l, w], s, nbr[l])

    def share(b, j, l, w):
        u = slot(b, j, 2 * c + l, w)
        return remote(u, u, fsem.at[b, j, l, w], rsem.at[b, j, 2 * c + l, w], s, sib)

    def arrived(b, j, k, w):
        u = slot(b, j, k, w)
        remote(u, u, fsem.at[b, j, 0, w], rsem.at[b, j, k, w], s, sib).wait_recv()

    def helped(w):
        return (s < S - 1) if w < 2 else (s == 1)

    def helper(w):
        return (s > 0) if w < 2 else (s == 2)

    def go_up(l, w):
        return remote(slot(1, 0, 2 * c + 1 - l, w), up[w].at[l], ssem.at[1, 1, l, w], usem.at[l, w], s + 1, tp)

    def go_over(l, w):
        return remote(up[w].at[l], over[w].at[l], oss.at[l, w], ovsem.at[l, w], s, nbr[l])

    def go_down(l, w):
        return remote(over[w].at[l], slot(1, 2, 2 * c + l, w), dss.at[l, w], rsem.at[1, 2, 2 * c + l, w], s - 1, tp)

    def each_part(cond, body):
        for w in range(3):
            @pl.when(cond(w))
            def _(w=w):
                for l in range(2):
                    body(l, w)

    def rows_of(i):
        return pl.ds(pl.multiple_of(i * CHUNK, CHUNK), CHUNK)

    def zsend(i):
        r = rows_of(i)
        return remote(y_ref.at[r], inbuf.at[r], zssem.at[i], zrsem.at[i], s + 1, tp)

    def each(n, body):
        def step(i, carry):
            body(i)
            return carry
        lax.fori_loop(0, n, step, 0)

    xin = pltpu.make_async_copy(x_hbm, inbuf, xsem)
    for b in range(NB):
        for q, w in LW:
            load(b, q, w).start()

    @pl.when(s == 0)
    def _():
        xin.start()

    barrier = pltpu.get_barrier_semaphore()
    for to in (sib, *nbr):
        pl.semaphore_signal(barrier, inc=1, device_id=(s, to), device_id_type=MESH)

    @pl.when(s > 0)
    def _():
        pl.semaphore_signal(barrier, inc=1, device_id=(s - 1, tp), device_id_type=MESH)

    @pl.when(s < S - 1)
    def _():
        pl.semaphore_signal(barrier, inc=1, device_id=(s + 1, tp), device_id_type=MESH)
    edge = (s == 0) | (s == S - 1)

    @pl.when(edge)
    def _():
        pl.semaphore_wait(barrier, 4)

    @pl.when(jnp.logical_not(edge))
    def _():
        pl.semaphore_wait(barrier, 5)

    for l, w in LW:
        load(0, l, w).wait()
    for j in (1, 2):
        for l, w in LW:
            send(0, j, l, w).start()
    for l, w in LW:
        load(1, l, w).wait()
    each_part(helped, lambda l, w: go_up(l, w).start())
    for b in range(NB):
        for l, w in LW:
            share(b, 0, l, w).start()

    def own_next():
        for l, w in LW:
            send(1, 1, l, w).start()

        each_part(lambda w: jnp.logical_not(helped(w)), lambda l, w: send(1, 2, l, w).start())

    def relay(b, j, on):
        for l, w in LW:
            arrived(b, j, 2 * c + l, w)
            if on:
                send(b, 3, 1 - l, w).start()
            share(b, j, l, w).start()
            if (b, j, l, w) == (0, 3, 1, 0):
                own_next()

    def others(b, j):
        for l, w in LW:
            arrived(b, j, 2 * (1 - c) + l, w)

    def norm(r0, n, b, src):
        g = g_ref[0, pl.ds(b, 1), :].astype(jnp.float32)
        for r in range(0, n, ROWS):
            rows = pl.ds(r0 + r, ROWS)
            yf = src[rows, :].astype(jnp.bfloat16).astype(jnp.float32)
            acc[rows, :] = yf
            yc = yf - jnp.mean(yf, axis=-1, keepdims=True)
            var = jnp.mean(jnp.square(yc), axis=-1, keepdims=True)
            hbuf[rows, :] = (yc * lax.rsqrt(var + EPS) * g).astype(jnp.bfloat16)

    def mlp(rows, b, j0, steps, final=False):
        h = hbuf[rows, :]
        n = steps * 4 * U
        for i in range(steps):
            for k in range(4):
                z = jnp.dot(h, w1v[b, j0 + i, k], preferred_element_type=jnp.float32)
                abuf[:rows.size, (4 * i + k) * U:(4 * i + k + 1) * U] = jax.nn.gelu(z).astype(jnp.bfloat16)
        w2 = w2v[b, j0] if steps == 1 else w2v[b, j0:j0 + steps].reshape(n, D)
        total = acc[rows, :] + jnp.dot(abuf[:rows.size, :n], w2, preferred_element_type=jnp.float32)
        if final:
            y_ref[rows, :] = total.astype(jnp.bfloat16)
        else:
            acc[rows, :] = total

    @pl.when(s == 0)
    def _():
        xin.wait()
        each(R // WIDE, lambda i: norm(pl.multiple_of(i * WIDE, WIDE), WIDE, 0, inbuf))

        def events(b, j):
            if j and (b, j) != (1, 1):
                relay(b, j, j == 1)
            others(b, j)

        def step(t):
            b, j = t // 4, t % 4
            for e in range(4 * NB - 1):
                @pl.when(t == e)
                def _(e=e):
                    events(e // 4, e % 4)

            def wide(i):
                @pl.when((t == 4) & (i == R // WIDE // 2))
                def _():
                    relay(1, 1, True)
                mlp(pl.ds(pl.multiple_of(i * WIDE, WIDE), WIDE), b, j, 1)
            each(R // WIDE, wide)

            @pl.when(t == 3)
            def _():
                each(R // WIDE, lambda i: norm(pl.multiple_of(i * WIDE, WIDE), WIDE, 1, acc))
        each(4 * NB - 1, step)
        events(NB - 1, 3)

        lag = LAG * c

        def last(i):
            mlp(rows_of(i), NB - 1, 3, 1, final=True)

            @pl.when(i >= lag)
            def _():
                zsend(i - lag).start()
        each(R // CHUNK, last)

        @pl.when(c == 1)
        def _():
            each(LAG, lambda i: zsend(R // CHUNK - LAG + i).start())

    @pl.when(s > 0)
    def _():
        relay(0, 1, False)
        def over_(l, w):
            go_up(l, w).wait_recv()
            go_over(l, w).start()

        def down_(l, w):
            go_over(l, w).wait_recv()
            go_down(l, w).start()
        each_part(helper, over_)
        for l, w in LW:
            send(0, 3, l, w).start()
        relay(0, 2, False)
        each_part(helper, down_)
        relay(0, 3, False)
        relay(1, 1, True)
        relay(1, 2, False)
        relay(1, 3, False)
        for b in range(NB):
            for j in range(4):
                others(b, j)

        def body(i):
            zsend(i).wait_recv()
            rows = rows_of(i)
            for b in range(NB):
                norm(rows.start, CHUNK, b, inbuf if b == 0 else acc)
                mlp(rows, b, 0, 4, final=b == NB - 1)

            @pl.when(s < S - 1)
            def _():
                zsend(i).start()
        each(R // CHUNK, body)

    for b in range(NB):
        for j in range(4):
            for l, w in LW:
                share(b, j, l, w).wait_send()
                if j:
                    send(b, j, l, w).wait_send()

    def helped_on(l, w):
        go_over(l, w).wait_send()
        go_down(l, w).wait_send()
    each_part(helper, helped_on)

    @pl.when(s < S - 1)
    def _():
        each(R // CHUNK, lambda i: zsend(i).wait_send())


def solution(mesh):
    S = mesh.shape['stage']

    def local(x, g, w1, w2):
        M, T, D = x.shape
        R = M * T
        n = R // CHUNK
        NB, F = w1.shape[1], w1.shape[3]
        U = F // 2
        bf, f32 = jnp.bfloat16, jnp.float32
        dma = pltpu.SemaphoreType.DMA
        y = pl.pallas_call(
            functools.partial(_kernel, S=S),
            out_shape=pltpu.VMEM((R, D), bf),
            in_specs=[pl.BlockSpec(memory_space=pl.ANY), pl.BlockSpec(memory_space=pltpu.VMEM),
                      pl.BlockSpec(memory_space=pl.ANY), pl.BlockSpec(memory_space=pl.ANY)],
            out_specs=pl.BlockSpec(memory_space=pltpu.VMEM),
            scratch_shapes=[
                pltpu.VMEM((NB, 4, 4, D, U), bf), pltpu.VMEM((NB, 4, 4 * U, D), bf),
                pltpu.VMEM((R, D), bf), pltpu.VMEM((R, D), bf),
                pltpu.VMEM((R, D), f32), pltpu.VMEM((WIDE, 16 * U), bf),
                *([pltpu.VMEM((2, D, U), bf)] + [pltpu.VMEM((2, U // 2, D), bf)] * 2) * 2,
                dma(()), dma((NB, 2, 3)), dma((NB, 4, 4, 3)), dma((NB, 3, 2, 3)), dma((NB, 4, 2, 3)),
                dma((2, 3)), dma((2, 3)), dma((2, 3)), dma((2, 3)),
                dma((n,)), dma((n,)),
            ],
            compiler_params=pltpu.CompilerParams(
                collective_id=0, has_side_effects=True, vmem_limit_bytes=62 * 1000 * 1000),
        )(x.reshape(R, D), g, w1, w2)
        return y.reshape(1, M, T, D)

    return jax.shard_map(
        local, mesh=mesh,
        in_specs=(P(None, 'tp', None), P('stage', None, None),
                  P('stage', None, None, 'tp'), P('stage', None, 'tp', None)),
        out_specs=P('stage', None, 'tp', None), check_vma=False)
```
